32 devices in a mesh: ga: 16 (over z, y, x), band: 2 (over core).
Axes of the slice: x: 2, y: 2, z: 4, core: 2. Of those that a mesh axis runs over, the one named last changes fastest.
Arguments:
- psi: bfloat16 [65536, 2048], P('ga', 'band'), may hold values from -1 to 1
- trial: bfloat16 [65536, 256], P('ga', 'band'), may hold values from -1.25 to 1.25
- beta: bfloat16 [65536, 1536], P('ga'), may hold values from -0.0625 to 0.0625
- q_blocks: float32 [128, 18, 18], replicated, may hold values from -6 to 6
- atom_counts: int32 [128], replicated, may hold values from 1 to 18, 1536 in all
Outputs:
- intersection: float32 [2048, 256], P('band', 'ga')
The draws below stay inside these ranges and needn't reach their ends.
Inputs may be any that keep to these rules, and one draw needn't show every extreme that they name: `atom_counts`: the counts sum to 1536; atoms own consecutive projectors in order, and some atom has exactly 18.
All inputs are finite; a program needn't handle non-finite values.
Results may differ from the reference program's by a relative error of at most 0.0003.
Values may be sent and summed in bfloat16 or wider, within the bound.
A program may use at most 64 MiB of HBM per device.

```python
import math
import jax
import jax.numpy as jnp
import numpy as np
from jax import lax

NG = 65536
NB = 2048
BLK = 256
P_SIZE = 1536
NATOM = 128
MAXP = 18


def spiked(drawn, stream_key, source, target, parts, factor):
    def block_of(axis_at):
        return (jnp.arange(drawn.shape[axis_at]) // (drawn.shape[axis_at] // parts)).reshape((-1,) + (1,) * (drawn.ndim - 1 - axis_at))

    first = jax.random.permutation(stream_key, parts)[block_of(target)]
    second = (block_of(target) + parts // 2) % parts
    return jnp.where((block_of(source) == first) | (block_of(source) == second), factor * drawn, drawn)


def levels(own_key, extent, shards, low, high):
    def one(dim, blocks):
        heights = jax.random.uniform(jax.random.fold_in(jax.random.fold_in(own_key, 6), dim), (blocks,), jnp.float32, low / len(shards), high / len(shards))
        return jnp.repeat(jnp.exp(heights), extent[dim] // blocks).reshape((-1,) + (1,) * (len(extent) - dim - 1))

    gain = one(*shards[0])
    for cut in shards[1:]:
        gain = gain * one(*cut)
    return gain


def profile(count, total, most, slope):
    weights = [(1 << 20) // math.isqrt(grade ** slope) + 1 for grade in range(2, count + 1)]
    spare, counts = total - most - (count - 1), [1] * (count - 1)
    while spare > 0:
        candidates = [i for i in range(count - 1) if counts[i] < most]
        mass, remaining = sum([weights[i] for i in candidates]), spare
        for i in candidates:
            addition = min(most - counts[i], max(1, remaining * weights[i] // mass), spare)
            counts[i] = counts[i] + addition
            spare = spare - addition
    return np.array([most] + counts)


def uneven_parts(rng, number_of, total, reach, lean):
    if number_of == 2:
        one = jax.random.randint(rng, (), max(1, total - reach), min(reach, total - 1) + 1)
        return jnp.stack([one, total - one])
    tallies = jnp.asarray(profile(number_of, total, reach, lean), jnp.int32)
    pairs = (number_of - 1) // 2
    donor, taker = tallies[1:1 + 2 * pairs:2], tallies[2:2 + 2 * pairs:2]
    slack = jnp.minimum(donor - 1, reach - taker)
    passed = jax.random.randint(jax.random.fold_in(rng, 1), (pairs,), 0, 1 << 20) % (slack + 1)
    tallies = tallies.at[1:1 + 2 * pairs:2].set(donor - passed).at[2:2 + 2 * pairs:2].set(taker + passed)
    return tallies[jax.random.permutation(jax.random.fold_in(rng, 2), number_of)]


def normal_values(key, dims, width, bound, pieces=(), held_as=jnp.bfloat16):
    values = width * jax.random.normal(key, dims, jnp.float32)
    if pieces:
        values = values * levels(key, dims, pieces, -0.22, 0.18)
    return jnp.clip(values, -bound, bound).astype(held_as)


def bell_draw_with(own_key, shape, scale, limit, pieces, heavy, kind=jnp.bfloat16):
    drawn = scale * jax.random.normal(own_key, shape, jnp.float32)
    if pieces:
        drawn = drawn * levels(own_key, shape, pieces, -0.22, 0.18)
    return jnp.clip(spiked(drawn, jax.random.fold_in(own_key, 3), *heavy), -limit, limit).astype(kind)


def setup_inputs(seed: int = 0) -> dict:
    seeds = jax.random.split(jax.random.key(seed), 6)
    return {
        "psi": normal_values(seeds[0], (NG, NB), (NG ** -0.25), 1.0, ((0, 16), (1, 2))),
        "trial": bell_draw_with(seeds[1], (NG, BLK), (NG ** -0.25), 1.25, ((0, 16), (1, 2)), (0, 1, 16, 2.0)),
        "beta": normal_values(seeds[2], (NG, P_SIZE), ((P_SIZE * MAXP * NG) ** -0.25), 0.0625, ((0, 16),)),
        "q_blocks": normal_values(seeds[3], (NATOM, MAXP, MAXP), 1.0, 6.0, (), jnp.float32),
        "atom_counts": uneven_parts(seeds[4], NATOM, P_SIZE, MAXP, 1).astype(jnp.int32),
    }


def contract(left, right, precision=None):
    return lax.dot_general(left, right, (((0,), (0,)), ((), ())), precision=precision, preferred_element_type=jnp.float32)


def reference(psi, trial, beta, q_blocks, atom_counts):
    offsets = jnp.cumsum(atom_counts, dtype=jnp.int32) - atom_counts
    ids = jnp.arange(P_SIZE, dtype=jnp.int32)
    below = offsets[None, :] <= ids[:, None]
    atom_ids = jnp.sum(below.astype(jnp.int32), axis=1, dtype=jnp.int32) - 1
    starts = jnp.max(jnp.where(below, offsets[None, :], 0), axis=1)
    position = ids - starts
    same_atom = atom_ids[:, None] == atom_ids[None, :]
    entries = q_blocks[atom_ids[:, None], position[:, None], position[None, :]]
    q_matrix = jnp.where(same_atom, entries, jnp.zeros_like(entries))
    proj_bands = contract(beta, psi)
    proj_trial = contract(beta, trial)
    weighted = jnp.dot(q_matrix, proj_trial, precision=lax.Precision.HIGHEST, preferred_element_type=jnp.float32)
    plain = contract(psi, trial)
    return plain + contract(proj_bands, weighted, lax.Precision.HIGHEST)
```

```python
import functools

import jax
import jax.numpy as jnp
from jax import lax
from jax.experimental import pallas as pl
from jax.experimental.pallas import tpu as pltpu
from jax.sharding import PartitionSpec as P

MESH = pl.DeviceIdType.MESH
precise = lax.Precision.HIGHEST
F32, BF16, I16 = jnp.float32, jnp.bfloat16, jnp.int16
LEVELS, TINY = 32767.0, 1e-30


def contract(left, right, precision=None):
    return lax.dot_general(
        left, right, (((0,), (0,)), ((), ())), precision=precision, preferred_element_type=F32
    )


def split2(x):
    hi = x.astype(BF16)
    return hi, (x - hi.astype(F32)).astype(BF16)


def encode(x):
    top = jnp.maximum(jnp.max(jnp.abs(x), keepdims=True), TINY)
    return jnp.round(x * (LEVELS / top)).astype(jnp.int32).astype(I16), top * (1.0 / LEVELS)


def decode(code, scale):
    return code.astype(jnp.int32).astype(F32) * scale


def kernel(
    n, inner, maxp, psi_h, trial_h, beta_h, q_ref, cnt_ref, out_ref,
    psi_v, beta_v, trial_v, beta_t, trial_t, q_parts, qd, g_hi, g_lo, w_hi, w_lo,
    proj, code1, scale1, in1, in1s, mid1, code1b, scale1b, end1, end1s,
    wall, walls, fin, code3, scale3, in3, in3s, mid3, code3b, scale3b, end3, end3s,
    trial_sem, beta_sem, psi_sem, xs, xr,
    send1, recv1, send1b, recv1b, send2, recv2, send2b, recv2b, send2c, recv2c,
    send3, recv3, send3b, recv3b,
):
    me = lax.axis_index("ga")
    band = lax.axis_index("band")
    outer = n // inner
    w, z = lax.rem(me, inner), lax.div(me, inner)

    def mate(d):
        return lax.rem(w + d, inner)

    def far(e):
        return lax.rem(z + e, outer)

    def reach(to_z, to_w):
        return dict(device_id=(to_z * inner + to_w, band), device_id_type=MESH)

    partner = dict(device_id=(me, 1 - band), device_id_type=MESH)

    g, cols = trial_v.shape
    p_size = beta_v.shape[1]
    nbands = psi_v.shape[1]
    natom = cnt_ref.shape[1]
    mp = q_ref.shape[0] // maxp
    r1 = cols // n
    r2 = out_ref.shape[0]
    beta_chunks = beta_sem.shape[0]
    bw = p_size // beta_chunks
    psi_chunks = psi_sem.shape[0]
    pw = nbands // psi_chunks
    sw = 512

    def aligned(i, size):
        return pl.ds(i * size if isinstance(i, int) else pl.multiple_of(i * size, size), size)

    def beta_copy(c):
        at = (slice(None), pl.ds(c * bw, bw))
        return pltpu.make_async_copy(beta_h.at[at], beta_v.at[at], beta_sem.at[c])

    def psi_copy(c):
        at = (slice(None), pl.ds(c * pw, pw))
        return pltpu.make_async_copy(psi_h.at[at], psi_v.at[at], psi_sem.at[c])

    trial_copy = pltpu.make_async_copy(trial_h, trial_v, trial_sem)
    trial_copy.start()
    for c in range(beta_chunks):
        beta_copy(c).start()
    for c in range(psi_chunks):
        psi_copy(c).start()

    barrier = pltpu.get_barrier_semaphore()

    for d in range(1, inner):
        pl.semaphore_signal(barrier, inc=1, **reach(z, mate(d)))
    for e in range(1, outer):
        pl.semaphore_signal(barrier, inc=1, **reach(far(e), w))
    pl.semaphore_signal(barrier, inc=1, **partner)

    class Pair:
        def __init__(self, src, src_s, dst, dst_s, send, recv, to):
            self.both = [
                pltpu.make_async_remote_copy(
                    src_ref=a, dst_ref=b, send_sem=send.at[i], recv_sem=recv.at[i], **to
                )
                for i, (a, b) in enumerate(((src, dst), (src_s, dst_s)))
            ]

        def start(self):
            for copy in self.both:
                copy.start()

        def wait(self):
            for copy in self.both:
                copy.wait()

    def inner1(c, d):
        at = pl.ds(c * bw, bw)
        return Pair(
            code1.at[aligned(mate(d), outer * r1), at], scale1.at[c],
            in1.at[d, :, at], in1s.at[c, d],
            send1.at[c, d], recv1.at[c, d], reach(z, mate(d)),
        )

    def outer1(c, e):
        at = pl.ds(c * bw, bw)
        return Pair(
            code1b.at[far(e), :, at], scale1b.at[c],
            end1.at[e, :, at], end1s.at[c, e],
            send1b.at[c, e], recv1b.at[c, e], reach(far(e), w),
        )

    def middle1(c):
        at = pl.ds(c * bw, bw)
        total = proj[aligned(w, outer * r1), at]
        for d in range(1, inner):
            inner1(c, d).wait()
            total += decode(in1[d, :, at], in1s[c, d][:, :1])
        code, scale = encode(total)
        scale1b[c] = jnp.broadcast_to(scale, (1, 128))
        code1b[:, :, at] = code.reshape(outer, r1, bw)
        mid1[:, :, at] = total.reshape(outer, r1, bw)
        for e in range(1, outer):
            outer1(c, e).start()

    def diagonals(c, _):
        lanes = 256
        nd = qd.shape[0]
        ids = (c * lanes + lax.broadcasted_iota(jnp.int32, (natom, lanes), 1)).astype(F32)
        owns = (offs <= ids) & (ids < offs + own)
        pos = jnp.sum(jnp.where(owns, ids - offs, 0.0), axis=0, keepdims=True)
        count = jnp.sum(jnp.where(owns, jnp.broadcast_to(own, owns.shape), 0.0), axis=0, keepdims=True)
        pick = jnp.where(owns, 1.0, 0.0).astype(BF16)
        flat = jnp.dot(q_parts[0], pick, preferred_element_type=F32)
        flat += jnp.dot(q_parts[1], pick, preferred_element_type=F32)
        flat += jnp.dot(q_parts[2], pick, preferred_element_type=F32)
        q_row = jnp.zeros((mp, lanes), F32)
        for i in range(maxp):
            q_row += jnp.where(pos == float(i), flat[i * mp : (i + 1) * mp], 0.0)
        at = pos + lax.broadcasted_iota(jnp.int32, (nd, lanes), 0).astype(F32) - float(maxp - 1)
        entries = jnp.zeros((nd, lanes), F32)
        for j in range(maxp):
            entries += jnp.where(at == float(j), q_row[j : j + 1], 0.0)
        qd[:, aligned(c, lanes)] = jnp.where(at < count, entries, 0.0)
        return 0

    trial_copy.wait()

    def turn(k, _):
        trial_t[aligned(band, cols), aligned(k, sw)] = trial_v[aligned(k, sw), :].T
        return 0

    lax.fori_loop(0, g // sw, turn, 0)

    pl.semaphore_wait(barrier, inner + outer - 1)

    trial_x = pltpu.make_async_remote_copy(
        src_ref=trial_t.at[aligned(band, cols), :],
        dst_ref=trial_t.at[aligned(band, cols), :],
        send_sem=xs,
        recv_sem=xr,
        **partner,
    )
    trial_x.start()

    for c in range(beta_chunks):
        beta_copy(c).wait()
        at = pl.ds(c * bw, bw)
        part = jnp.dot(
            trial_t[aligned(band, cols), :], beta_v[:, at], preferred_element_type=F32
        )
        proj[:, at] = part
        code, scale = encode(part)
        code1[:, at] = code
        scale1[c] = jnp.broadcast_to(scale, (1, 128))
        for d in range(1, inner):
            inner1(c, d).start()

    def flip(c):
        def piece(k, _):
            beta_t[pl.ds(c * bw, bw), aligned(k, sw)] = beta_v[aligned(k, sw), pl.ds(c * bw, bw)].T
            return 0

        lax.fori_loop(0, g // sw, piece, 0)

    flip(0)

    cnt = cnt_ref[...].astype(F32)
    row = lax.broadcasted_iota(jnp.int32, (natom, natom), 0)
    col = lax.broadcasted_iota(jnp.int32, (natom, natom), 1)
    offs = jnp.sum(jnp.where(col < row, cnt, 0.0), axis=1, keepdims=True)
    own = jnp.sum(jnp.where(col == row, cnt, 0.0), axis=1, keepdims=True)
    q = q_ref[...]
    q_hi = q.astype(BF16)
    rest = q - q_hi.astype(F32)
    q_mid = rest.astype(BF16)
    q_parts[0] = q_hi
    q_parts[1] = q_mid
    q_parts[2] = (rest - q_mid.astype(F32)).astype(BF16)
    lax.fori_loop(0, p_size // 256, diagonals, 0)

    middle1(0)

    trial_x.wait()
    for c in range(psi_chunks):
        psi_copy(c).wait()

    def plain(c, _):
        got = jnp.dot(trial_t[...], psi_v[:, aligned(c, pw)], preferred_element_type=F32)
        fin[:, :, :, aligned(c, pw)] = got.reshape(outer, inner, r2, pw)
        return 0

    def bands(c):
        def piece(k, _):
            at = (pl.ds(c * bw, bw), aligned(k, pw))
            got = jnp.dot(
                beta_t[pl.ds(c * bw, bw), :], psi_v[:, aligned(k, pw)], preferred_element_type=F32
            )
            hi, lo = split2(got)
            g_hi[at] = hi
            g_lo[at] = lo
            return 0

        lax.fori_loop(0, psi_chunks, piece, 0)

    lax.fori_loop(0, psi_chunks, plain, 0)
    for c in range(1, beta_chunks):
        middle1(c)

    bands(0)

    for c in range(beta_chunks):
        for e in range(1, outer):
            outer1(c, e).wait()
    pieces = []
    for c in range(beta_chunks):
        at = pl.ds(c * bw, bw)
        piece = mid1[z, :, at]
        for e in range(1, outer):
            piece += decode(end1[e, :, at], end1s[c, e][:, :1])
        pieces.append(piece)
    x = jnp.concatenate(pieces, axis=1)
    acc = jnp.zeros_like(x)
    for d in range(2 * maxp - 1):
        shift = (maxp - 1 - d) % p_size
        moved = x if shift == 0 else pltpu.roll(x, shift, axis=1)
        acc += qd[d : d + 1, :] * moved
    mine = w * outer + z
    code, scale = encode(acc)
    wall[band, mine] = code
    walls[band, mine] = jnp.broadcast_to(scale, (1, 128))

    def outer2(e):
        return Pair(
            wall.at[band, mine], walls.at[band, mine], wall.at[band, mine], walls.at[band, mine],
            send2.at[e], recv2.at[e], reach(far(e), w),
        )

    def inner2(e, d):
        block = w * outer + lax.rem(z + outer - e, outer)
        return Pair(
            wall.at[band, block], walls.at[band, block], wall.at[band, block], walls.at[band, block],
            send2b.at[e, d], recv2b.at[e, d], reach(z, mate(d)),
        )

    def across(d):
        rows = aligned(lax.rem(w + inner - d, inner), outer)
        return Pair(
            wall.at[band, rows], walls.at[band, rows], wall.at[band, rows], walls.at[band, rows],
            send2c.at[d], recv2c.at[d], partner,
        )

    for e in range(1, outer):
        outer2(e).start()
    for d in range(1, inner):
        inner2(0, d).start()

    flip(1)
    bands(1)
    for e in range(1, outer):
        outer2(e).wait()
        for d in range(1, inner):
            inner2(e, d).start()
    across(0).start()
    flip(2)
    bands(2)

    for d in range(1, inner):
        for e in range(outer):
            inner2(e, d).wait()
        across(d).start()
    for d in range(inner):
        across(d).wait()

    def spread(i, _):
        for b in range(2):
            both = [decode(wall[b, 2 * i + j], walls[b, 2 * i + j][:, :1]) for j in range(2)]
            hi, lo = split2(jnp.concatenate(both, axis=0))
            at = pl.ds(pl.multiple_of(b * cols + i * 2 * r1, 2 * r1), 2 * r1)
            w_hi[at, :] = hi
            w_lo[at, :] = lo
        return 0

    lax.fori_loop(0, n // 2, spread, 0)

    def inner3(c, d):
        return Pair(
            code3.at[:, mate(d), :, aligned(c, pw)], scale3.at[c],
            in3.at[d, :, :, aligned(c, pw)], in3s.at[c, d],
            send3.at[c, d], recv3.at[c, d], reach(z, mate(d)),
        )

    def outer3(c, e):
        return Pair(
            code3b.at[far(e), :, aligned(c, pw)], scale3b.at[c],
            end3.at[e, :, aligned(c, pw)], end3s.at[c, e],
            send3b.at[c, e], recv3b.at[c, e], reach(far(e), w),
        )

    def middle3(c):
        at = aligned(c, pw)
        for d in range(1, inner):
            inner3(c, d).wait()
        total = fin[:, w, :, at].reshape(outer * r2, pw)
        for d in range(1, inner):
            total += decode(in3[d, :, :, at].reshape(outer * r2, pw), in3s[c, d][:, :1])
        code, scale = encode(total)
        scale3b[c] = jnp.broadcast_to(scale, (1, 128))
        code3b[:, :, at] = code.reshape(outer, r2, pw)
        mid3[:, :, at] = total.reshape(outer, r2, pw)
        for e in range(1, outer):
            outer3(c, e).start()

    def share(c):
        at = aligned(c, pw)
        f = jnp.dot(w_hi[...], g_hi[:, at], preferred_element_type=F32)
        f += jnp.dot(w_hi[...], g_lo[:, at], preferred_element_type=F32)
        f += jnp.dot(w_lo[...], g_hi[:, at], preferred_element_type=F32)
        f += fin[:, :, :, at].reshape(2 * cols, pw)
        code, scale = encode(f)
        scale3[c] = jnp.broadcast_to(scale, (1, 128))
        code3[:, :, :, at] = code.reshape(outer, inner, r2, pw)
        fin[:, :, :, at] = f.reshape(outer, inner, r2, pw)
        for d in range(1, inner):
            inner3(c, d).start()

    for c in range(psi_chunks):
        share(c)
        if c:
            middle3(c - 1)
    middle3(psi_chunks - 1)

    for c in range(psi_chunks):
        at = aligned(c, pw)
        total = mid3[z, :, at]
        for e in range(1, outer):
            outer3(c, e).wait()
            total += decode(end3[e, :, at], end3s[c, e][:, :1])
        out_ref[:, at] = total


def fused(n, inner, blk, psi, trial, beta, q_blocks, atom_counts):
    g, cols = trial.shape
    nbands = psi.shape[1]
    p_size = beta.shape[1]
    natom, maxp = q_blocks.shape[:2]
    mp = -(-maxp // 8) * 8
    nd = -(-(2 * maxp - 1) // 8) * 8
    r1, r2 = cols // n, blk // n
    outer = n // inner
    bc, pc = 3, 4
    q_flat = jnp.pad(q_blocks, ((0, 0), (0, 0), (0, mp - maxp)))
    q_flat = q_flat.transpose(1, 2, 0).reshape(maxp * mp, natom)
    dma = pltpu.SemaphoreType.DMA
    vm = pltpu.VMEM
    out = pl.pallas_call(
        functools.partial(kernel, n, inner, maxp),
        out_shape=jax.ShapeDtypeStruct((r2, nbands), F32),
        in_specs=[pl.BlockSpec(memory_space=pl.ANY)] * 3
        + [pl.BlockSpec(memory_space=pltpu.VMEM)] * 2,
        out_specs=pl.BlockSpec(memory_space=pltpu.VMEM),
        scratch_shapes=[
            vm((g, nbands), BF16),
            vm((g, p_size), BF16),
            vm((g, cols), BF16),
            vm((p_size, g), BF16),
            vm((blk, g), BF16),
            vm((3, maxp * mp, natom), BF16),
            vm((nd, p_size), F32),
            vm((p_size, nbands), BF16),
            vm((p_size, nbands), BF16),
            vm((blk, p_size), BF16),
            vm((blk, p_size), BF16),
            vm((cols, p_size), F32),
            vm((cols, p_size), I16),
            vm((bc, 1, 128), F32),
            vm((inner, outer * r1, p_size), I16),
            vm((bc, inner, 1, 128), F32),
            vm((outer, r1, p_size), F32),
            vm((outer, r1, p_size), I16),
            vm((bc, 1, 128), F32),
            vm((outer, r1, p_size), I16),
            vm((bc, outer, 1, 128), F32),
            vm((2, n, r1, p_size), I16),
            vm((2, n, 1, 128), F32),
            vm((outer, inner, r2, nbands), F32),
            vm((outer, inner, r2, nbands), I16),
            vm((pc, 1, 128), F32),
            vm((inner, outer, r2, nbands), I16),
            vm((pc, inner, 1, 128), F32),
            vm((outer, r2, nbands), F32),
            vm((outer, r2, nbands), I16),
            vm((pc, 1, 128), F32),
            vm((outer, r2, nbands), I16),
            vm((pc, outer, 1, 128), F32),
            dma,
            dma((bc,)),
            dma((pc,)),
            dma,
            dma,
            dma((bc, inner, 2)),
            dma((bc, inner, 2)),
            dma((bc, outer, 2)),
            dma((bc, outer, 2)),
            dma((outer, 2)),
            dma((outer, 2)),
            dma((outer, inner, 2)),
            dma((outer, inner, 2)),
            dma((inner, 2)),
            dma((inner, 2)),
            dma((pc, inner, 2)),
            dma((pc, inner, 2)),
            dma((pc, outer, 2)),
            dma((pc, outer, 2)),
        ],
        compiler_params=pltpu.CompilerParams(
            collective_id=0, has_side_effects=True, vmem_limit_bytes=62 * 1024 * 1024
        ),
    )(psi, trial, beta, q_flat, atom_counts.reshape(1, natom))
    return out.T


def q_dense(atom_counts, q_blocks, p_size):
    offsets = jnp.cumsum(atom_counts, dtype=jnp.int32) - atom_counts
    natom, maxp = q_blocks.shape[:2]
    ids = jnp.arange(p_size, dtype=jnp.int32)
    owns = (offsets[None, :] <= ids[:, None]) & (ids[:, None] < (offsets + atom_counts)[None, :])
    pos = jnp.sum(jnp.where(owns, ids[:, None] - offsets[None, :], 0), axis=1)
    atom = jnp.sum(jnp.where(owns, jnp.arange(natom, dtype=jnp.int32)[None, :], 0), axis=1)
    flat = jnp.dot(owns.astype(F32), q_blocks.reshape(natom, maxp * maxp), precision=precise)
    place = pos[:, None] == jnp.arange(maxp, dtype=jnp.int32)[None, :]
    rows = jnp.sum(jnp.where(place[:, :, None], flat.reshape(p_size, maxp, maxp), 0.0), axis=1)
    entries = jnp.dot(rows, place.astype(F32).T, precision=precise)
    return jnp.where(atom[:, None] == atom[None, :], entries, 0.0)


def general(psi, trial, beta, q_blocks, atom_counts):
    own = lax.psum(contract(beta, trial), "ga")
    weighted = jnp.dot(q_dense(atom_counts, q_blocks, beta.shape[1]), own, precision=precise)
    w_hi, w_lo = split2(weighted)
    both = jnp.dot(beta, jnp.concatenate([w_hi, w_lo], axis=1), preferred_element_type=F32)
    cols = trial.shape[1]
    s = both[:, :cols] + both[:, cols:] + trial.astype(F32)
    s_hi, s_lo = split2(lax.all_gather(s, "band", axis=1, tiled=True))
    part = contract(psi, s_hi) + contract(psi, s_lo)
    return lax.psum_scatter(part, "ga", scatter_dimension=1, tiled=True)


def solution(mesh):
    n, bands = mesh.shape["ga"], mesh.shape["band"]
    inner = 4

    def shards(psi, trial, beta, q_blocks, atom_counts):
        g, cols = trial.shape
        blk = cols * bands
        fits = (
            bands == 2
            and n % (2 * inner) == 0
            and cols % 128 == 0
            and cols % (8 * n) == 0
            and blk % (8 * n) == 0
            and g % 4096 == 0
            and beta.shape[1] % 768 == 0
            and psi.shape[1] % 512 == 0
            and q_blocks.shape[0] % 128 == 0
        )
        if fits:
            return fused(n, inner, blk, psi, trial, beta, q_blocks, atom_counts)
        return general(psi, trial, beta, q_blocks, atom_counts)

    in_specs = (P("ga", "band"), P("ga", "band"), P("ga", None), P(), P())
    out_specs = P("band", "ga")
    return jax.shard_map(shards, mesh=mesh, in_specs=in_specs, out_specs=out_specs, check_vma=False)
```

```python
import functools

import jax
import jax.numpy as jnp
from jax import lax
from jax.experimental import pallas as pl
from jax.experimental.pallas import tpu as pltpu
from jax.sharding import PartitionSpec as P

MESH = pl.DeviceIdType.MESH
precise = lax.Precision.HIGHEST
F32, BF16, I16 = jnp.float32, jnp.bfloat16, jnp.int16
LEVELS, TINY = 32767.0, 1e-30


def contract(left, right, precision=None):
    return lax.dot_general(
        left, right, (((0,), (0,)), ((), ())), precision=precision, preferred_element_type=F32
    )


def split2(x):
    hi = x.astype(BF16)
    return hi, (x - hi.astype(F32)).astype(BF16)


def encode(x):
    top = jnp.maximum(jnp.max(jnp.abs(x), keepdims=True), TINY)
    return jnp.round(x * (LEVELS / top)).astype(jnp.int32).astype(I16), top * (1.0 / LEVELS)


def decode(code, scale):
    return code.astype(jnp.int32).astype(F32) * scale


def kernel(
    n, inner, maxp, psi_h, trial_h, beta_h, q_h, cnt_h, out_ref,
    psi_v, beta_v, trial_v, q_v, cnt_v, beta_t, trial_t, q_parts, qd, g_hi, g_lo, w_hi, w_lo,
    proj, code1, scale1, in1, in1s, mid1, code1b, scale1b, end1, end1s,
    wall, walls, fin, code3, scale3, in3, in3s, mid3, code3b, scale3b, end3, end3s,
    q_sem, trial_sem, beta_sem, psi_sem, xs, xr, sent, recv1, recv1b, recv2, recv2b, recv2c,
    recv3, recv3b,
):
    me = lax.axis_index("ga")
    band = lax.axis_index("band")
    outer = n // inner
    w, z = lax.rem(me, inner), lax.div(me, inner)

    def mate(d):
        x, y = lax.rem(w, 2), lax.div(w, 2)
        return lax.rem(x + d % 2, 2) + 2 * lax.rem(y + d // 2, 2)

    def far(e):
        return lax.rem(z + e, outer)

    def reach(to_z, to_w):
        return dict(device_id=(to_z * inner + to_w, band), device_id_type=MESH)

    partner = dict(device_id=(me, 1 - band), device_id_type=MESH)
    mates = tuple(range(inner - 1, 0, -1))
    fars = tuple(range(1, outer))

    g, cols = trial_v.shape
    p_size = beta_v.shape[1]
    nbands = psi_v.shape[1]
    natom = cnt_v.shape[1]
    mp = q_parts.shape[1] // maxp
    r1 = cols // n
    r2 = out_ref.shape[0]
    beta_chunks = beta_sem.shape[0]
    bw = p_size // beta_chunks
    psi_chunks = psi_sem.shape[0]
    pw = nbands // psi_chunks
    sw = 512

    def aligned(i, size):
        return pl.ds(i * size if isinstance(i, int) else pl.multiple_of(i * size, size), size)

    def beta_copy(c):
        at = (slice(None), pl.ds(c * bw, bw))
        return pltpu.make_async_copy(beta_h.at[at], beta_v.at[at], beta_sem.at[c])

    def psi_copy(c):
        at = (slice(None), pl.ds(c * pw, pw))
        return pltpu.make_async_copy(psi_h.at[at], psi_v.at[at], psi_sem.at[c])

    q_copy = pltpu.make_async_copy(q_h, q_v, q_sem.at[0])
    cnt_copy = pltpu.make_async_copy(cnt_h, cnt_v, q_sem.at[1])
    trial_copy = pltpu.make_async_copy(trial_h, trial_v, trial_sem)
    q_copy.start()
    cnt_copy.start()
    trial_copy.start()
    beta_copy(0).start()

    barrier = pltpu.get_barrier_semaphore()

    for d in mates:
        pl.semaphore_signal(barrier, inc=1, **reach(z, mate(d)))
    for e in fars:
        pl.semaphore_signal(barrier, inc=1, **reach(far(e), w))
    pl.semaphore_signal(barrier, inc=1, **partner)

    def send(stage, src, src_s, dst, dst_s, recv, to):
        for i, (a, b) in enumerate(((src, dst), (src_s, dst_s))):
            pltpu.make_async_remote_copy(
                src_ref=a, dst_ref=b, send_sem=sent.at[stage, i], recv_sem=recv.at[i], **to
            ).start()

    def landed(ref, ref_s, recv):
        for i, a in enumerate((ref, ref_s)):
            pltpu.make_async_remote_copy(
                src_ref=a, dst_ref=a, send_sem=sent.at[0, i], recv_sem=recv.at[i], **partner
            ).wait_recv()

    def left(stage, ref, ref_s):
        for i, a in enumerate((ref, ref_s)):
            pltpu.make_async_remote_copy(
                src_ref=a, dst_ref=a, send_sem=sent.at[stage, i], recv_sem=recv1.at[0, i], **partner
            ).wait_send()

    def middle1(c):
        at = pl.ds(c * bw, bw)
        landed(in1.at[pl.ds(1, inner - 1), :, at], in1s.at[c, pl.ds(1, inner - 1)], recv1.at[c])
        total = proj[aligned(w, outer * r1), at]
        for d in mates:
            total += decode(in1[d, :, at], in1s[c, d][:, :1])
        code, scale = encode(total)
        scale1b[c] = jnp.broadcast_to(scale, (1, 128))
        code1b[:, :, at] = code.reshape(outer, r1, bw)
        mid1[:, :, at] = total.reshape(outer, r1, bw)
        for e in fars:
            send(
                1, code1b.at[far(e), :, at], scale1b.at[c],
                end1.at[e, :, at], end1s.at[c, e], recv1b.at[c], reach(far(e), w),
            )

    with jax.named_scope("q_wait"):
        q_copy.wait()
        cnt_copy.wait()
    with jax.named_scope("diag"):
        cnt = cnt_v[...].astype(F32)
        row = lax.broadcasted_iota(jnp.int32, (natom, natom), 0)
        col = lax.broadcasted_iota(jnp.int32, (natom, natom), 1)
        offs = jnp.sum(jnp.where(col < row, cnt, 0.0), axis=1, keepdims=True)
        own = jnp.sum(jnp.where(col == row, cnt, 0.0), axis=1, keepdims=True)
        q_parts[...] = jnp.zeros_like(q_parts)
        for i in range(maxp):
            q = q_v[i]
            q_hi = q.astype(BF16)
            rest = q - q_hi.astype(F32)
            q_mid = rest.astype(BF16)
            at = slice(i * mp, i * mp + maxp)
            q_parts[0, at] = q_hi
            q_parts[1, at] = q_mid
            q_parts[2, at] = (rest - q_mid.astype(F32)).astype(BF16)

        def diagonals(c, _):
            lanes = 256
            nd = qd.shape[0]
            ids = (c * lanes + lax.broadcasted_iota(jnp.int32, (natom, lanes), 1)).astype(F32)
            owns = (offs <= ids) & (ids < offs + own)
            pos = jnp.sum(jnp.where(owns, ids - offs, 0.0), axis=0, keepdims=True)
            count = jnp.sum(
                jnp.where(owns, jnp.broadcast_to(own, owns.shape), 0.0), axis=0, keepdims=True
            )
            pick = jnp.where(owns, 1.0, 0.0).astype(BF16)
            flat = jnp.dot(q_parts[0], pick, preferred_element_type=F32)
            flat += jnp.dot(q_parts[1], pick, preferred_element_type=F32)
            flat += jnp.dot(q_parts[2], pick, preferred_element_type=F32)
            q_row = jnp.zeros((mp, lanes), F32)
            for i in range(maxp):
                q_row += jnp.where(pos == float(i), flat[i * mp : (i + 1) * mp], 0.0)
            at = pos + lax.broadcasted_iota(jnp.int32, (nd, lanes), 0).astype(F32) - float(maxp - 1)
            entries = jnp.zeros((nd, lanes), F32)
            for j in range(maxp):
                entries += jnp.where(at == float(j), q_row[j : j + 1], 0.0)
            qd[:, aligned(c, lanes)] = jnp.where(at < count, entries, 0.0)
            return 0

        lax.fori_loop(0, p_size // 256, diagonals, 0)

    with jax.named_scope("trial_wait"):
        trial_copy.wait()
    beta_copy(1).start()

    def turn(k, _):
        trial_t[aligned(band, cols), aligned(k, sw)] = trial_v[aligned(k, sw), :].T
        return 0

    with jax.named_scope("turn"):
        lax.fori_loop(0, g // sw, turn, 0)

    with jax.named_scope("barrier"):
        pl.semaphore_wait(barrier, inner + outer - 1)

    trial_x = pltpu.make_async_remote_copy(
        src_ref=trial_t.at[aligned(band, cols), :],
        dst_ref=trial_t.at[aligned(band, cols), :],
        send_sem=xs,
        recv_sem=xr,
        **partner,
    )
    trial_x.start()

    for c in range(beta_chunks):
        with jax.named_scope(f"load_{c}"):
            beta_copy(c).wait()
        if c + 2 < beta_chunks:
            beta_copy(c + 2).start()
        elif c + 2 == beta_chunks:
            for k in range(psi_chunks):
                psi_copy(k).start()
        at = pl.ds(c * bw, bw)
        with jax.named_scope(f"p1_{c}"):
            part = jnp.dot(
                trial_t[aligned(band, cols), :], beta_v[:, at], preferred_element_type=F32
            )
            proj[:, at] = part
            code, scale = encode(part)
            code1[:, at] = code
            scale1[c] = jnp.broadcast_to(scale, (1, 128))
            for d in mates:
                send(
                    0, code1.at[aligned(mate(d), outer * r1), at], scale1.at[c],
                    in1.at[d, :, at], in1s.at[c, d], recv1.at[c], reach(z, mate(d)),
                )

    def flip(c):
        def piece(k, _):
            beta_t[pl.ds(c * bw, bw), aligned(k, sw)] = beta_v[aligned(k, sw), pl.ds(c * bw, bw)].T
            return 0

        with jax.named_scope(f"flip_{c}"):
            lax.fori_loop(0, g // sw, piece, 0)

    def plain(c, _):
        got = jnp.dot(trial_t[...], psi_v[:, aligned(c, pw)], preferred_element_type=F32)
        fin[:, :, :, aligned(c, pw)] = got.reshape(outer, inner, r2, pw)
        return 0

    def bands(c):
        step = bw // psi_chunks

        def piece(k, _):
            at = (pl.ds(c * bw, bw), aligned(k, pw))
            if c + 1 < beta_chunks:
                part = pl.ds(pl.multiple_of((c + 1) * bw + k * step, step), step)
                beta_t[part, :] = beta_v[:, part].T
            got = jnp.dot(
                beta_t[pl.ds(c * bw, bw), :], psi_v[:, aligned(k, pw)], preferred_element_type=F32
            )
            hi, lo = split2(got)
            g_hi[at] = hi
            g_lo[at] = lo
            return 0

        with jax.named_scope(f"bands_{c}"):
            lax.fori_loop(0, psi_chunks, piece, 0)

    flip(0)
    with jax.named_scope("psi_wait"):
        trial_x.wait()
        for c in range(psi_chunks):
            psi_copy(c).wait()
    with jax.named_scope("plain"):
        lax.fori_loop(0, psi_chunks, plain, 0)
    for c in range(beta_chunks):
        with jax.named_scope(f"mid1_{c}"):
            middle1(c)
    bands(0)

    with jax.named_scope("wait_z1"):
        for c in range(beta_chunks):
            at = pl.ds(c * bw, bw)
            landed(
                end1.at[pl.ds(1, outer - 1), :, at], end1s.at[c, pl.ds(1, outer - 1)], recv1b.at[c]
            )

    mine = w * outer + z
    with jax.named_scope("q_apply"):
        pieces = []
        for c in range(beta_chunks):
            at = pl.ds(c * bw, bw)
            piece = mid1[z, :, at]
            for e in fars:
                piece += decode(end1[e, :, at], end1s[c, e][:, :1])
            pieces.append(piece)
        x = jnp.concatenate(pieces, axis=1)
        acc = jnp.zeros_like(x)
        for d in range(2 * maxp - 1):
            shift = (maxp - 1 - d) % p_size
            moved = x if shift == 0 else pltpu.roll(x, shift, axis=1)
            acc += qd[d : d + 1, :] * moved
        code, scale = encode(acc)
        wall[band, mine] = code
        walls[band, mine] = jnp.broadcast_to(scale, (1, 128))

    def share_w(stage, rows, recv, to):
        a, b = wall.at[band, rows], walls.at[band, rows]
        send(stage, a, b, a, b, recv, to)

    for e in fars:
        share_w(2, mine, recv2.at[e - 1], reach(far(e), w))
    for d in mates:
        share_w(3, mine, recv2b.at[d - 1], reach(z, mate(d)))

    bands(1)
    with jax.named_scope("ag_z"):
        for e in fars:
            block = w * outer + lax.rem(z + outer - e, outer)
            landed(wall.at[band, block], walls.at[band, block], recv2.at[e - 1])
            for d in mates:
                share_w(3, block, recv2b.at[d - 1], reach(z, mate(d)))
        share_w(4, aligned(w, outer), recv2c.at[0], partner)
    bands(2)

    with jax.named_scope("ag_xy"):
        for d in (1, 2, 3):
            rows = aligned(mate(d), outer)
            landed(wall.at[band, rows], walls.at[band, rows], recv2b.at[d - 1])
            share_w(4, rows, recv2c.at[d], partner)
        for d in range(inner):
            rows = aligned(mate(d), outer)
            landed(wall.at[1 - band, rows], walls.at[1 - band, rows], recv2c.at[d])

    def spread(i, _):
        for b in range(2):
            both = [decode(wall[b, 2 * i + j], walls[b, 2 * i + j][:, :1]) for j in range(2)]
            hi, lo = split2(jnp.concatenate(both, axis=0))
            at = pl.ds(pl.multiple_of(b * cols + i * 2 * r1, 2 * r1), 2 * r1)
            w_hi[at, :] = hi
            w_lo[at, :] = lo
        return 0

    with jax.named_scope("spread"):
        lax.fori_loop(0, n // 2, spread, 0)

    def middle3(c):
        at = aligned(c, pw)
        others = pl.ds(1, inner - 1)
        landed(in3.at[others, :, :, at], in3s.at[c, others], recv3.at[c])
        total = fin[:, w, :, at].reshape(outer * r2, pw)
        for d in mates:
            total += decode(in3[d, :, :, at].reshape(outer * r2, pw), in3s[c, d][:, :1])
        code, scale = encode(total)
        scale3b[c] = jnp.broadcast_to(scale, (1, 128))
        code3b[:, :, at] = code.reshape(outer, r2, pw)
        mid3[:, :, at] = total.reshape(outer, r2, pw)
        for e in fars:
            send(
                6, code3b.at[far(e), :, at], scale3b.at[c],
                end3.at[e, :, at], end3s.at[c, e], recv3b.at[c], reach(far(e), w),
            )

    def share(c):
        at = aligned(c, pw)
        f = jnp.dot(w_hi[...], g_hi[:, at], preferred_element_type=F32)
        f += jnp.dot(w_hi[...], g_lo[:, at], preferred_element_type=F32)
        f += jnp.dot(w_lo[...], g_hi[:, at], preferred_element_type=F32)
        f += fin[:, :, :, at].reshape(2 * cols, pw)
        code, scale = encode(f)
        scale3[c] = jnp.broadcast_to(scale, (1, 128))
        code3[:, :, :, at] = code.reshape(outer, inner, r2, pw)
        fin[:, :, :, at] = f.reshape(outer, inner, r2, pw)
        for d in mates:
            send(
                5, code3.at[:, mate(d), :, at], scale3.at[c],
                in3.at[d, :, :, at], in3s.at[c, d], recv3.at[c], reach(z, mate(d)),
            )

    for c in range(psi_chunks):
        with jax.named_scope(f"share_{c}"):
            share(c)
    for c in range(psi_chunks):
        with jax.named_scope(f"mid3_{c}"):
            middle3(c)

    with jax.named_scope("tail"):
        others = pl.ds(1, outer - 1)
        for c in range(psi_chunks):
            at = aligned(c, pw)
            landed(end3.at[others, :, at], end3s.at[c, others], recv3b.at[c])
            total = mid3[z, :, at]
            for e in fars:
                total += decode(end3[e, :, at], end3s[c, e][:, :1])
            out_ref[:, at] = total

    with jax.named_scope("drain"):
        k, m = pl.ds(0, inner - 1), pl.ds(0, outer - 1)
        left(0, code1.at[pl.ds(0, (inner - 1) * outer * r1), :], in1s.at[:, k])
        left(1, code1b.at[m], end1s.at[:, m])
        left(2, wall.at[0, m], walls.at[0, m])
        rows = pl.ds(0, (inner - 1) * outer)
        left(3, wall.at[0, rows], walls.at[0, rows])
        left(4, wall.at[0], walls.at[0])
        left(5, code3.at[:, k], in3s.at[:, k])
        left(6, code3b.at[m], end3s.at[:, m])


def fused(n, inner, blk, psi, trial, beta, q_blocks, atom_counts):
    g, cols = trial.shape
    nbands = psi.shape[1]
    p_size = beta.shape[1]
    natom, maxp = q_blocks.shape[:2]
    mp = -(-maxp // 8) * 8
    nd = -(-(2 * maxp - 1) // 8) * 8
    r1, r2 = cols // n, blk // n
    outer = n // inner
    bc, pc = 3, 4
    dma = pltpu.SemaphoreType.DMA
    vm = pltpu.VMEM
    out = pl.pallas_call(
        functools.partial(kernel, n, inner, maxp),
        out_shape=jax.ShapeDtypeStruct((r2, nbands), F32),
        in_specs=[pl.BlockSpec(memory_space=pl.ANY)] * 5,
        out_specs=pl.BlockSpec(memory_space=pltpu.VMEM),
        scratch_shapes=[
            vm((g, nbands), BF16),
            vm((g, p_size), BF16),
            vm((g, cols), BF16),
            vm((maxp, maxp, natom), F32),
            vm((1, natom), jnp.int32),
            vm((p_size, g), BF16),
            vm((blk, g), BF16),
            vm((3, maxp * mp, natom), BF16),
            vm((nd, p_size), F32),
            vm((p_size, nbands), BF16),
            vm((p_size, nbands), BF16),
            vm((blk, p_size), BF16),
            vm((blk, p_size), BF16),
            vm((cols, p_size), F32),
            vm((cols, p_size), I16),
            vm((bc, 1, 128), F32),
            vm((inner, outer * r1, p_size), I16),
            vm((bc, inner, 1, 128), F32),
            vm((outer, r1, p_size), F32),
            vm((outer, r1, p_size), I16),
            vm((bc, 1, 128), F32),
            vm((outer, r1, p_size), I16),
            vm((bc, outer, 1, 128), F32),
            vm((2, n, r1, p_size), I16),
            vm((2, n, 1, 128), F32),
            vm((outer, inner, r2, nbands), F32),
            vm((outer, inner, r2, nbands), I16),
            vm((pc, 1, 128), F32),
            vm((inner, outer, r2, nbands), I16),
            vm((pc, inner, 1, 128), F32),
            vm((outer, r2, nbands), F32),
            vm((outer, r2, nbands), I16),
            vm((pc, 1, 128), F32),
            vm((outer, r2, nbands), I16),
            vm((pc, outer, 1, 128), F32),
            dma((2,)),
            dma,
            dma((bc,)),
            dma((pc,)),
            dma,
            dma,
            dma((7, 2)),
            dma((bc, 2)),
            dma((bc, 2)),
            dma((outer - 1, 2)),
            dma((inner - 1, 2)),
            dma((inner, 2)),
            dma((pc, 2)),
            dma((pc, 2)),
        ],
        compiler_params=pltpu.CompilerParams(
            collective_id=0, has_side_effects=True, vmem_limit_bytes=62 * 1024 * 1024
        ),
    )(psi, trial, beta, q_blocks.transpose(1, 2, 0), atom_counts.reshape(1, natom))
    return out.T


def q_dense(atom_counts, q_blocks, p_size):
    offsets = jnp.cumsum(atom_counts, dtype=jnp.int32) - atom_counts
    natom, maxp = q_blocks.shape[:2]
    ids = jnp.arange(p_size, dtype=jnp.int32)
    owns = (offsets[None, :] <= ids[:, None]) & (ids[:, None] < (offsets + atom_counts)[None, :])
    pos = jnp.sum(jnp.where(owns, ids[:, None] - offsets[None, :], 0), axis=1)
    atom = jnp.sum(jnp.where(owns, jnp.arange(natom, dtype=jnp.int32)[None, :], 0), axis=1)
    flat = jnp.dot(owns.astype(F32), q_blocks.reshape(natom, maxp * maxp), precision=precise)
    place = pos[:, None] == jnp.arange(maxp, dtype=jnp.int32)[None, :]
    rows = jnp.sum(jnp.where(place[:, :, None], flat.reshape(p_size, maxp, maxp), 0.0), axis=1)
    entries = jnp.dot(rows, place.astype(F32).T, precision=precise)
    return jnp.where(atom[:, None] == atom[None, :], entries, 0.0)


def general(psi, trial, beta, q_blocks, atom_counts):
    own = lax.psum(contract(beta, trial), "ga")
    weighted = jnp.dot(q_dense(atom_counts, q_blocks, beta.shape[1]), own, precision=precise)
    w_hi, w_lo = split2(weighted)
    both = jnp.dot(beta, jnp.concatenate([w_hi, w_lo], axis=1), preferred_element_type=F32)
    cols = trial.shape[1]
    s = both[:, :cols] + both[:, cols:] + trial.astype(F32)
    s_hi, s_lo = split2(lax.all_gather(s, "band", axis=1, tiled=True))
    part = contract(psi, s_hi) + contract(psi, s_lo)
    return lax.psum_scatter(part, "ga", scatter_dimension=1, tiled=True)


def solution(mesh):
    n, bands = mesh.shape["ga"], mesh.shape["band"]
    inner = 4

    def shards(psi, trial, beta, q_blocks, atom_counts):
        g, cols = trial.shape
        blk = cols * bands
        fits = (
            bands == 2
            and n % (2 * inner) == 0
            and cols % 128 == 0
            and cols % (8 * n) == 0
            and blk % (8 * n) == 0
            and g % 4096 == 0
            and beta.shape[1] % 768 == 0
            and psi.shape[1] % 512 == 0
            and q_blocks.shape[0] % 128 == 0
        )
        if fits:
            return fused(n, inner, blk, psi, trial, beta, q_blocks, atom_counts)
        return general(psi, trial, beta, q_blocks, atom_counts)

    in_specs = (P("ga", "band"), P("ga", "band"), P("ga", None), P(), P())
    out_specs = P("band", "ga")
    return jax.shard_map(shards, mesh=mesh, in_specs=in_specs, out_specs=out_specs, check_vma=False)
```

```python
import functools

import jax
import jax.numpy as jnp
from jax import lax
from jax.experimental import pallas as pl
from jax.experimental.pallas import tpu as pltpu
from jax.sharding import PartitionSpec as P

MESH = pl.DeviceIdType.MESH
precise = lax.Precision.HIGHEST
F32, BF16, I16 = jnp.float32, jnp.bfloat16, jnp.int16
LEVELS, TINY = 32767.0, 1e-30


def contract(left, right, precision=None):
    return lax.dot_general(
        left, right, (((0,), (0,)), ((), ())), precision=precision, preferred_element_type=F32
    )


def split2(x):
    hi = x.astype(BF16)
    return hi, (x - hi.astype(F32)).astype(BF16)


def encode(x):
    top = jnp.maximum(jnp.max(jnp.abs(x), keepdims=True), TINY)
    return jnp.round(x * (LEVELS / top)).astype(jnp.int32).astype(I16), top * (1.0 / LEVELS)


def decode(code, scale):
    return code.astype(jnp.int32).astype(F32) * scale


def kernel(
    n, maxp, psi_h, trial_h, beta_h, q_h, cnt_h, out_ref,
    psi_v, beta_v, trial_v, q_v, cnt_v, beta_t0, beta_t1, beta_t2, trial_t, q_parts, qd, g_hi, g_lo, w_hi, w_lo,
    proj, code1, scale1, in1, in1s, mid1, code1b, scale1b, end1, end1s,
    wall, walls, fin, code3, scale3, in3, in3s, mid3, code3b, scale3b, end3, end3s,
    q_sem, trial_sem, beta_sem, psi_sem, xs, xr, sent, recv1, recv1b, recv2, recv2b, recv2c,
    recv3, recv3b,
):
    me = lax.axis_index("ga")
    band = lax.axis_index("band")
    bit = [lax.rem(lax.div(me, 1 << p), 2) for p in range(4)]
    routes = (((1, 0), (3, 2)), ((2, 1), (3, 0)), ((2, 0), (3, 1)))
    peers = (3, 2, 1)

    def toggled(pair, d):
        return {p: lax.rem(bit[p] + (d >> k & 1), 2) for k, p in enumerate(pair[::-1])}

    def device(pair, d):
        there = sum((v - bit[p]) * (1 << p) for p, v in toggled(pair, d).items())
        return dict(device_id=(me + there, band), device_id_type=MESH)

    def pick(pair, d):
        bits = toggled(pair, d)
        return tuple(bits.get(p, slice(None)) for p in (3, 2, 1, 0))

    def cell(pair, d):
        bits = toggled(pair, d)
        return tuple(bits[p] for p in pair)

    partner = dict(device_id=(me, 1 - band), device_id_type=MESH)

    g, cols = trial_v.shape
    p_size = beta_v.shape[1]
    nbands = psi_v.shape[1]
    natom = cnt_v.shape[1]
    mp = q_parts.shape[1] // maxp
    r1 = cols // n
    r2 = out_ref.shape[0]
    beta_chunks = beta_sem.shape[0]
    bw = p_size // beta_chunks
    psi_chunks = psi_sem.shape[0]
    pw = nbands // psi_chunks
    sw = 512
    beta_t = (beta_t0, beta_t1, beta_t2)

    def aligned(i, size):
        return pl.ds(i * size if isinstance(i, int) else pl.multiple_of(i * size, size), size)

    def beta_copy(c):
        at = (slice(None), pl.ds(c * bw, bw))
        return pltpu.make_async_copy(beta_h.at[at], beta_v.at[at], beta_sem.at[c])

    def psi_copy(c):
        at = (slice(None), pl.ds(c * pw, pw))
        return pltpu.make_async_copy(psi_h.at[at], psi_v.at[at], psi_sem.at[c])

    q_copy = pltpu.make_async_copy(q_h, q_v, q_sem.at[0])
    cnt_copy = pltpu.make_async_copy(cnt_h, cnt_v, q_sem.at[1])
    trial_copy = pltpu.make_async_copy(trial_h, trial_v, trial_sem)
    q_copy.start()
    cnt_copy.start()
    trial_copy.start()
    beta_copy(0).start()

    barrier = pltpu.get_barrier_semaphore()

    met = [(pair, d) for pair in routes[0] for d in peers]
    met += [(pair, 3) for route in routes[1:] for pair in route]
    for pair, d in met:
        pl.semaphore_signal(barrier, inc=1, **device(pair, d))
    pl.semaphore_signal(barrier, inc=1, **partner)

    def send(stage, src, src_s, dst, dst_s, recv, to):
        for i, (a, b) in enumerate(((src, dst), (src_s, dst_s))):
            pltpu.make_async_remote_copy(
                src_ref=a, dst_ref=b, send_sem=sent.at[stage, i], recv_sem=recv.at[i], **to
            ).start()

    def landed(ref, ref_s, recv):
        for i, a in enumerate((ref, ref_s)):
            pltpu.make_async_remote_copy(
                src_ref=a, dst_ref=a, send_sem=sent.at[0, i], recv_sem=recv.at[i], **partner
            ).wait_recv()

    def left(stage, ref, ref_s):
        for i, a in enumerate((ref, ref_s)):
            pltpu.make_async_remote_copy(
                src_ref=a, dst_ref=a, send_sem=sent.at[stage, i], recv_sem=recv1.at[0, i], **partner
            ).wait_send()

    others = pl.ds(1, 3)

    def middle1(c):
        near, late = routes[c % 3]
        at = pl.ds(c * bw, bw)
        landed(in1.at[others, :, :, :, at], in1s.at[c, others], recv1.at[c])
        total = proj[pick(near, 0) + (slice(None), at)].reshape(4 * r1, bw)
        for d in peers:
            total += decode(in1[d, :, :, :, at].reshape(4 * r1, bw), in1s[c, d][:, :1])
        code, scale = encode(total)
        scale1b[c] = jnp.broadcast_to(scale, (1, 128))
        code1b[:, :, :, at] = code.reshape(2, 2, r1, bw)
        mid1[:, :, :, at] = total.reshape(2, 2, r1, bw)
        for d in peers:
            send(
                1, code1b.at[cell(late, d) + (slice(None), at)], scale1b.at[c],
                end1.at[d, :, at], end1s.at[c, d], recv1b.at[c], device(late, d),
            )

    with jax.named_scope("q_wait"):
        q_copy.wait()
        cnt_copy.wait()
    beta_copy(1).start()
    with jax.named_scope("diag"):
        cnt = cnt_v[...].astype(F32)
        row = lax.broadcasted_iota(jnp.int32, (natom, natom), 0)
        col = lax.broadcasted_iota(jnp.int32, (natom, natom), 1)
        offs = jnp.sum(jnp.where(col < row, cnt, 0.0), axis=1, keepdims=True)
        own = jnp.sum(jnp.where(col == row, cnt, 0.0), axis=1, keepdims=True)
        q_parts[...] = jnp.zeros_like(q_parts)
        for i in range(maxp):
            q = q_v[i]
            q_hi = q.astype(BF16)
            rest = q - q_hi.astype(F32)
            q_mid = rest.astype(BF16)
            at = slice(i * mp, i * mp + maxp)
            q_parts[0, at] = q_hi
            q_parts[1, at] = q_mid
            q_parts[2, at] = (rest - q_mid.astype(F32)).astype(BF16)

        def diagonals(c, _):
            lanes = 256
            nd = qd.shape[0]
            ids = (c * lanes + lax.broadcasted_iota(jnp.int32, (natom, lanes), 1)).astype(F32)
            owns = (offs <= ids) & (ids < offs + own)
            pos = jnp.sum(jnp.where(owns, ids - offs, 0.0), axis=0, keepdims=True)
            count = jnp.sum(
                jnp.where(owns, jnp.broadcast_to(own, owns.shape), 0.0), axis=0, keepdims=True
            )
            pick = jnp.where(owns, 1.0, 0.0).astype(BF16)
            flat = jnp.dot(q_parts[0], pick, preferred_element_type=F32)
            flat += jnp.dot(q_parts[1], pick, preferred_element_type=F32)
            flat += jnp.dot(q_parts[2], pick, preferred_element_type=F32)
            q_row = jnp.zeros((mp, lanes), F32)
            for i in range(maxp):
                q_row += jnp.where(pos == float(i), flat[i * mp : (i + 1) * mp], 0.0)
            at = pos + lax.broadcasted_iota(jnp.int32, (nd, lanes), 0).astype(F32) - float(maxp - 1)
            entries = jnp.zeros((nd, lanes), F32)
            for j in range(maxp):
                entries += jnp.where(at == float(j), q_row[j : j + 1], 0.0)
            qd[:, aligned(c, lanes)] = jnp.where(at < count, entries, 0.0)
            return 0

        for c in range(p_size // 256):
            diagonals(c, 0)
            if c == 2:
                beta_copy(2).start()

    with jax.named_scope("trial_wait"):
        trial_copy.wait()
    psi_copy(0).start()

    def turn(k, _):
        trial_t[aligned(band, cols), aligned(k, sw)] = trial_v[aligned(k, sw), :].T
        return 0

    with jax.named_scope("turn"):
        for k in range(g // sw):
            turn(k, 0)

    trial_x = pltpu.make_async_remote_copy(
        src_ref=trial_t.at[aligned(band, cols), :],
        dst_ref=trial_t.at[aligned(band, cols), :],
        send_sem=xs,
        recv_sem=xr,
        **partner,
    )

    for c in range(beta_chunks):
        with jax.named_scope(f"load_{c}"):
            beta_copy(c).wait()
        at = pl.ds(c * bw, bw)
        with jax.named_scope(f"p1_{c}"):
            part = jnp.dot(
                trial_t[aligned(band, cols), :], beta_v[:, at], preferred_element_type=F32
            )
            code, scale = encode(part)
            proj[:, :, :, :, :, at] = part.reshape(2, 2, 2, 2, r1, bw)
            code1[:, :, :, :, :, at] = code.reshape(2, 2, 2, 2, r1, bw)
            scale1[c] = jnp.broadcast_to(scale, (1, 128))
            if c == 0:
                with jax.named_scope("barrier"):
                    pl.semaphore_wait(barrier, len(met) + 1)
                trial_x.start()
            near = routes[c % 3][0]
            for d in peers:
                send(
                    0, code1.at[pick(near, d) + (slice(None), at)], scale1.at[c],
                    in1.at[d, :, :, :, at], in1s.at[c, d], recv1.at[c], device(near, d),
                )
        for k in ((1,), (2, 3), ())[c]:
            psi_copy(k).start()

    step = bw // psi_chunks

    def flip(c, k):
        if c < beta_chunks:
            part = pl.ds(pl.multiple_of(c * bw + k * step, step), step)
            beta_t[c][aligned(k, step), :] = beta_v[:, part].T

    def plain(lo, hi):
        def piece(k, _):
            psi_copy(k).wait()
            flip(0, k)
            got = jnp.dot(trial_t[...], psi_v[:, aligned(k, pw)], preferred_element_type=F32)
            fin[..., aligned(k, pw)] = got.reshape(2, 2, 2, 2, r2, pw)
            return 0

        with jax.named_scope(f"plain_{lo}"):
            lax.fori_loop(lo, hi, piece, 0)

    def bands(c, lo, hi, turns=1):
        def piece(k, _):
            for j in range(turns):
                flip(c + 1, k * turns + j)
            got = jnp.dot(beta_t[c][...], psi_v[:, aligned(k, pw)], preferred_element_type=F32)
            top, rest = split2(got)
            at = (pl.ds(c * bw, bw), aligned(k, pw))
            g_hi[at] = top
            g_lo[at] = rest
            return 0

        with jax.named_scope(f"bands_{c}_{lo}"):
            lax.fori_loop(lo, hi, piece, 0)

    with jax.named_scope("trial_x"):
        trial_x.wait()
    plain(0, 4)
    for c in range(beta_chunks):
        with jax.named_scope(f"mid1_{c}"):
            middle1(c)
    bands(0, 0, 4)

    with jax.named_scope("wait_z1"):
        for c in range(beta_chunks):
            landed(end1.at[others, :, pl.ds(c * bw, bw)], end1s.at[c, others], recv1b.at[c])

    with jax.named_scope("q_apply"):
        pieces = []
        for c in range(beta_chunks):
            at = pl.ds(c * bw, bw)
            piece = mid1[cell(routes[c % 3][1], 0) + (slice(None), at)]
            for d in peers:
                piece += decode(end1[d, :, at], end1s[c, d][:, :1])
            pieces.append(piece)
        x = jnp.concatenate(pieces, axis=1)
        acc = jnp.zeros_like(x)
        for d in range(2 * maxp - 1):
            shift = (maxp - 1 - d) % p_size
            moved = x if shift == 0 else pltpu.roll(x, shift, axis=1)
            acc += qd[d : d + 1, :] * moved
        code, scale = encode(acc)
        wall[(band,) + pick((3, 2), 0)[:2] + pick((1, 0), 0)[2:]] = code
        walls[(band,) + pick((3, 2), 0)[:2] + pick((1, 0), 0)[2:]] = jnp.broadcast_to(
            scale, (1, 128)
        )

    plane, line = routes[0]

    def share_w(stage, at, recv, to):
        a, b = wall.at[at], walls.at[at]
        send(stage, a, b, a, b, recv, to)

    def block(d):
        return (band,) + cell(line, d) + cell(plane, 0)

    def column(b, d):
        return (b,) + pick(plane, d)

    for d in peers:
        share_w(2, block(0), recv2.at[d - 1], device(line, d))
    for d in peers:
        share_w(3, block(0), recv2b.at[d - 1], device(plane, d))

    def relay(e):
        landed(wall.at[block(e)], walls.at[block(e)], recv2.at[e - 1])
        for d in peers:
            share_w(3, block(e), recv2b.at[d - 1], device(plane, d))

    def spread(b, d):
        y, x = cell(plane, d)
        for i in range(2):
            for k in range(2):
                at = (b, i, k, y, x)
                top, rest = split2(decode(wall[at], walls[at][:, :1]))
                w_hi[at] = top
                w_lo[at] = rest

    bands(1, 0, 2, 2)
    with jax.named_scope("ag_z1"):
        relay(1)
    bands(1, 2, 3, 0)
    with jax.named_scope("ag_z2"):
        relay(2)
    bands(1, 3, 4, 0)
    with jax.named_scope("ag_z3"):
        relay(3)
        share_w(4, column(band, 0), recv2c.at[0], partner)
    bands(2, 0, 4)

    with jax.named_scope("ag_xy"):
        for d in (1, 2, 3):
            landed(wall.at[column(band, d)], walls.at[column(band, d)], recv2b.at[d - 1])
            share_w(4, column(band, d), recv2c.at[d], partner)
    with jax.named_scope("spread_own"):
        for d in range(4):
            spread(band, d)
    with jax.named_scope("across"):
        for d in range(4):
            at = column(1 - band, d)
            landed(wall.at[at], walls.at[at], recv2c.at[d])
            spread(1 - band, d)

    def middle3(c):
        near, late = routes[c % 3]
        at = aligned(c, pw)
        landed(in3.at[others, :, :, :, at], in3s.at[c, others], recv3.at[c])
        total = fin[pick(near, 0) + (slice(None), at)].reshape(4 * r2, pw)
        for d in peers:
            total += decode(in3[d, :, :, :, at].reshape(4 * r2, pw), in3s[c, d][:, :1])
        code, scale = encode(total)
        scale3b[c] = jnp.broadcast_to(scale, (1, 128))
        code3b[:, :, :, at] = code.reshape(2, 2, r2, pw)
        mid3[:, :, :, at] = total.reshape(2, 2, r2, pw)
        for d in peers:
            send(
                6, code3b.at[cell(late, d) + (slice(None), at)], scale3b.at[c],
                end3.at[d, :, at], end3s.at[c, d], recv3b.at[c], device(late, d),
            )

    def product(c):
        at = aligned(c, pw)
        hi = w_hi[...].reshape(2 * cols, p_size)
        f = jnp.dot(hi, g_hi[:, at], preferred_element_type=F32)
        f += jnp.dot(hi, g_lo[:, at], preferred_element_type=F32)
        f += jnp.dot(w_lo[...].reshape(2 * cols, p_size), g_hi[:, at], preferred_element_type=F32)
        return f + fin[..., at].reshape(2 * cols, pw)

    def share(c, f):
        near = routes[c % 3][0]
        at = aligned(c, pw)
        code, scale = encode(f)
        scale3[c] = jnp.broadcast_to(scale, (1, 128))
        code3[..., at] = code.reshape(2, 2, 2, 2, r2, pw)
        fin[..., at] = f.reshape(2, 2, 2, 2, r2, pw)
        for d in peers:
            send(
                5, code3.at[pick(near, d) + (slice(None), at)], scale3.at[c],
                in3.at[d, :, :, :, at], in3s.at[c, d], recv3.at[c], device(near, d),
            )

    with jax.named_scope("share"):
        f = product(0)
        for c in range(psi_chunks):
            later = product(c + 1) if c + 1 < psi_chunks else None
            share(c, f)
            f = later
    for c in range(psi_chunks):
        with jax.named_scope(f"mid3_{c}"):
            middle3(c)

    with jax.named_scope("tail"):
        for c in range(psi_chunks):
            at = aligned(c, pw)
            landed(end3.at[others, :, at], end3s.at[c, others], recv3b.at[c])
            total = mid3[cell(routes[c % 3][1], 0) + (slice(None), at)]
            for d in peers:
                total += decode(end3[d, :, at], end3s[c, d][:, :1])
            out_ref[:, at] = total

    with jax.named_scope("drain"):
        three = pl.ds(0, 3)
        left(0, in1.at[others], in1s.at[:, three])
        left(1, end1.at[others], end1s.at[:, three])
        left(2, end1.at[others], end1s.at[0, three])
        left(3, in1.at[others], in3s.at[three])
        left(4, wall.at[0], walls.at[0])
        left(5, in3.at[others], in3s.at[:, three])
        left(6, end3.at[others], end3s.at[:, three])


def fused(n, blk, psi, trial, beta, q_blocks, atom_counts):
    g, cols = trial.shape
    nbands = psi.shape[1]
    p_size = beta.shape[1]
    natom, maxp = q_blocks.shape[:2]
    mp = -(-maxp // 8) * 8
    nd = -(-(2 * maxp - 1) // 8) * 8
    r1, r2 = cols // n, blk // n
    bc, pc = 3, 4
    dma = pltpu.SemaphoreType.DMA
    vm = pltpu.VMEM
    out = pl.pallas_call(
        functools.partial(kernel, n, maxp),
        out_shape=jax.ShapeDtypeStruct((r2, nbands), F32),
        in_specs=[pl.BlockSpec(memory_space=pl.ANY)] * 5,
        out_specs=pl.BlockSpec(memory_space=pltpu.VMEM),
        scratch_shapes=[
            vm((g, nbands), BF16),
            vm((g, p_size), BF16),
            vm((g, cols), BF16),
            vm((maxp, maxp, natom), F32),
            vm((1, natom), jnp.int32),
            vm((p_size // bc, g), BF16),
            vm((p_size // bc, g), BF16),
            vm((p_size // bc, g), BF16),
            vm((blk, g), BF16),
            vm((3, maxp * mp, natom), BF16),
            vm((nd, p_size), F32),
            vm((p_size, nbands), BF16),
            vm((p_size, nbands), BF16),
            vm((2, 2, 2, 2, 2, r1, p_size), BF16),
            vm((2, 2, 2, 2, 2, r1, p_size), BF16),
            vm((2, 2, 2, 2, r1, p_size), F32),
            vm((2, 2, 2, 2, r1, p_size), I16),
            vm((bc, 1, 128), F32),
            vm((4, 2, 2, r1, p_size), I16),
            vm((bc, 4, 1, 128), F32),
            vm((2, 2, r1, p_size), F32),
            vm((2, 2, r1, p_size), I16),
            vm((bc, 1, 128), F32),
            vm((4, r1, p_size), I16),
            vm((bc, 4, 1, 128), F32),
            vm((2, 2, 2, 2, 2, r1, p_size), I16),
            vm((2, 2, 2, 2, 2, 1, 128), F32),
            vm((2, 2, 2, 2, r2, nbands), F32),
            vm((2, 2, 2, 2, r2, nbands), I16),
            vm((pc, 1, 128), F32),
            vm((4, 2, 2, r2, nbands), I16),
            vm((pc, 4, 1, 128), F32),
            vm((2, 2, r2, nbands), F32),
            vm((2, 2, r2, nbands), I16),
            vm((pc, 1, 128), F32),
            vm((4, r2, nbands), I16),
            vm((pc, 4, 1, 128), F32),
            dma((2,)),
            dma,
            dma((bc,)),
            dma((pc,)),
            dma,
            dma,
            dma((7, 2)),
            dma((bc, 2)),
            dma((bc, 2)),
            dma((3, 2)),
            dma((3, 2)),
            dma((4, 2)),
            dma((pc, 2)),
            dma((pc, 2)),
        ],
        compiler_params=pltpu.CompilerParams(
            collective_id=0, has_side_effects=True, vmem_limit_bytes=62 * 1024 * 1024
        ),
    )(psi, trial, beta, q_blocks.transpose(1, 2, 0), atom_counts.reshape(1, natom))
    return out.T


def q_dense(atom_counts, q_blocks, p_size):
    offsets = jnp.cumsum(atom_counts, dtype=jnp.int32) - atom_counts
    natom, maxp = q_blocks.shape[:2]
    ids = jnp.arange(p_size, dtype=jnp.int32)
    owns = (offsets[None, :] <= ids[:, None]) & (ids[:, None] < (offsets + atom_counts)[None, :])
    pos = jnp.sum(jnp.where(owns, ids[:, None] - offsets[None, :], 0), axis=1)
    atom = jnp.sum(jnp.where(owns, jnp.arange(natom, dtype=jnp.int32)[None, :], 0), axis=1)
    flat = jnp.dot(owns.astype(F32), q_blocks.reshape(natom, maxp * maxp), precision=precise)
    place = pos[:, None] == jnp.arange(maxp, dtype=jnp.int32)[None, :]
    rows = jnp.sum(jnp.where(place[:, :, None], flat.reshape(p_size, maxp, maxp), 0.0), axis=1)
    entries = jnp.dot(rows, place.astype(F32).T, precision=precise)
    return jnp.where(atom[:, None] == atom[None, :], entries, 0.0)


def general(psi, trial, beta, q_blocks, atom_counts):
    own = lax.psum(contract(beta, trial), "ga")
    weighted = jnp.dot(q_dense(atom_counts, q_blocks, beta.shape[1]), own, precision=precise)
    w_hi, w_lo = split2(weighted)
    both = jnp.dot(beta, jnp.concatenate([w_hi, w_lo], axis=1), preferred_element_type=F32)
    cols = trial.shape[1]
    s = both[:, :cols] + both[:, cols:] + trial.astype(F32)
    s_hi, s_lo = split2(lax.all_gather(s, "band", axis=1, tiled=True))
    part = contract(psi, s_hi) + contract(psi, s_lo)
    return lax.psum_scatter(part, "ga", scatter_dimension=1, tiled=True)


def solution(mesh):
    n, bands = mesh.shape["ga"], mesh.shape["band"]

    def shards(psi, trial, beta, q_blocks, atom_counts):
        g, cols = trial.shape
        blk = cols * bands
        fits = (
            bands == 2
            and n == 16
            and cols % 128 == 0
            and cols % (8 * n) == 0
            and blk % (8 * n) == 0
            and g % 4096 == 0
            and beta.shape[1] % 768 == 0
            and psi.shape[1] % 512 == 0
            and q_blocks.shape[0] % 128 == 0
        )
        if fits:
            return fused(n, blk, psi, trial, beta, q_blocks, atom_counts)
        return general(psi, trial, beta, q_blocks, atom_counts)

    in_specs = (P("ga", "band"), P("ga", "band"), P("ga", None), P(), P())
    out_specs = P("band", "ga")
    return jax.shard_map(shards, mesh=mesh, in_specs=in_specs, out_specs=out_specs, check_vma=False)
```

```python
import functools

import jax
import jax.numpy as jnp
from jax import lax
from jax.experimental import pallas as pl
from jax.experimental.pallas import tpu as pltpu
from jax.sharding import PartitionSpec as P

MESH = pl.DeviceIdType.MESH
precise = lax.Precision.HIGHEST
F32, BF16, I16 = jnp.float32, jnp.bfloat16, jnp.int16
LEVELS, TINY = 32767.0, 1e-30


def contract(left, right, precision=None):
    return lax.dot_general(
        left, right, (((0,), (0,)), ((), ())), precision=precision, preferred_element_type=F32
    )


def split2(x):
    hi = x.astype(BF16)
    return hi, (x - hi.astype(F32)).astype(BF16)


def encode(x):
    top = jnp.maximum(jnp.max(jnp.abs(x), keepdims=True), TINY)
    return jnp.round(x * (LEVELS / top)).astype(jnp.int32).astype(I16), top * (1.0 / LEVELS)


def decode(code, scale):
    return code.astype(jnp.int32).astype(F32) * scale


def kernel(
    n, maxp, psi_h, trial_h, beta_h, q_h, cnt_h, out_ref,
    psi_v, beta_v, trial_v, q_v, cnt_v, lhs, beta_t, trial_t, q_parts, qd, g_hi, g_lo, w_hi, w_lo,
    proj, code1, scale1, in1, in1s, mid1, code1b, scale1b, end1, end1s,
    wall, walls, fin, code3, scale3, in3, in3s, mid3, code3b, scale3b, end3, end3s, meter,
    q_sem, trial_sem, beta_sem, psi_sem, xs, xr, sent, recv1, recv1b, recv2, recv2b, recv2c,
    recv3, recv3b,
):
    me = lax.axis_index("ga")
    band = lax.axis_index("band")
    bit = [lax.rem(lax.div(me, 1 << p), 2) for p in range(4)]
    routes = (((1, 0), (3, 2)), ((2, 1), (3, 0)), ((2, 0), (3, 1)))
    peers = (3, 2, 1)

    def toggled(pair, d):
        return {p: lax.rem(bit[p] + (d >> k & 1), 2) for k, p in enumerate(pair[::-1])}

    def device(pair, d):
        there = sum((v - bit[p]) * (1 << p) for p, v in toggled(pair, d).items())
        return dict(device_id=(me + there, band), device_id_type=MESH)

    def pick(pair, d):
        bits = toggled(pair, d)
        return tuple(bits.get(p, slice(None)) for p in (3, 2, 1, 0))

    def cell(pair, d):
        bits = toggled(pair, d)
        return tuple(bits[p] for p in pair)

    partner = dict(device_id=(me, 1 - band), device_id_type=MESH)

    g, cols = trial_v.shape
    p_size = beta_v.shape[1]
    nbands = psi_v.shape[1]
    natom = cnt_v.shape[1]
    mp = q_parts.shape[1] // maxp
    r1 = cols // n
    r2 = out_ref.shape[0]
    beta_chunks = beta_sem.shape[0]
    bw = p_size // beta_chunks
    psi_chunks = psi_sem.shape[0]
    pw = nbands // psi_chunks
    sw = 512

    def aligned(i, size):
        return pl.ds(i * size if isinstance(i, int) else pl.multiple_of(i * size, size), size)

    def beta_copy(c):
        at = (slice(None), pl.ds(c * bw, bw))
        return pltpu.make_async_copy(beta_h.at[at], beta_v.at[at], beta_sem.at[c])

    def psi_copy(c):
        at = (slice(None), pl.ds(c * pw, pw))
        return pltpu.make_async_copy(psi_h.at[at], psi_v.at[at], psi_sem.at[c])

    q_copy = pltpu.make_async_copy(q_h, q_v, q_sem.at[0])
    cnt_copy = pltpu.make_async_copy(cnt_h, cnt_v, q_sem.at[1])
    trial_copy = pltpu.make_async_copy(trial_h, trial_v, trial_sem)
    q_copy.start()
    cnt_copy.start()
    trial_copy.start()
    beta_copy(0).start()

    barrier = pltpu.get_barrier_semaphore()

    met = [(pair, d) for pair in routes[0] for d in peers]
    met += [(pair, 3) for route in routes[1:] for pair in route]
    for pair, d in met:
        pl.semaphore_signal(barrier, inc=1, **device(pair, d))
    pl.semaphore_signal(barrier, inc=1, **partner)

    def send(src, src_s, dst, dst_s, recv, to):
        for a, b in ((src, dst), (src_s, dst_s)):
            pltpu.make_async_remote_copy(
                src_ref=a, dst_ref=b, send_sem=sent, recv_sem=recv, **to
            ).start()

    def size(values, copies):
        return copies * (2 * values + 4 * 128) // (4 * 128)

    def counted(rows, recv):
        a = meter.at[pl.ds(0, rows)]
        return pltpu.make_async_remote_copy(
            src_ref=a, dst_ref=a, send_sem=sent, recv_sem=recv, **partner
        )

    def landed(rows, recv):
        counted(rows, recv).wait_recv()

    near1, late1 = size(4 * r1 * bw, 3), size(r1 * bw, 3)
    near3, late3 = size(4 * r2 * pw, 3), size(r2 * pw, 3)
    one = size(r1 * p_size, 1)

    def middle1(c):
        near, late = routes[c % 3]
        at = pl.ds(c * bw, bw)
        landed(near1, recv1.at[c])
        total = proj[pick(near, 0) + (slice(None), at)].reshape(4 * r1, bw)
        for d in peers:
            total += decode(in1[d, :, :, :, at].reshape(4 * r1, bw), in1s[c, d][:, :1])
        code, scale = encode(total)
        scale1b[c] = jnp.broadcast_to(scale, (1, 128))
        code1b[:, :, :, at] = code.reshape(2, 2, r1, bw)
        mid1[:, :, :, at] = total.reshape(2, 2, r1, bw)
        for d in peers:
            send(
                code1b.at[cell(late, d) + (slice(None), at)], scale1b.at[c],
                end1.at[d, :, at], end1s.at[c, d], recv1b.at[c], device(late, d),
            )

    with jax.named_scope("q_wait"):
        q_copy.wait()
        cnt_copy.wait()
    beta_copy(1).start()
    with jax.named_scope("diag"):
        cnt = cnt_v[...].astype(F32)
        row = lax.broadcasted_iota(jnp.int32, (natom, natom), 0)
        col = lax.broadcasted_iota(jnp.int32, (natom, natom), 1)
        offs = jnp.sum(jnp.where(col < row, cnt, 0.0), axis=1, keepdims=True)
        own = jnp.sum(jnp.where(col == row, cnt, 0.0), axis=1, keepdims=True)
        q_parts[...] = jnp.zeros_like(q_parts)
        for i in range(maxp):
            q = q_v[i]
            q_hi = q.astype(BF16)
            at = slice(i * mp, i * mp + maxp)
            q_parts[0, at] = q_hi
            q_parts[1, at] = (q - q_hi.astype(F32)).astype(BF16)

        def diagonals(c, _):
            lanes = 256
            nd = qd.shape[0]
            ids = (c * lanes + lax.broadcasted_iota(jnp.int32, (natom, lanes), 1)).astype(F32)
            owns = (offs <= ids) & (ids < offs + own)
            pos = jnp.sum(jnp.where(owns, ids - offs, 0.0), axis=0, keepdims=True)
            count = jnp.sum(
                jnp.where(owns, jnp.broadcast_to(own, owns.shape), 0.0), axis=0, keepdims=True
            )
            pick = jnp.where(owns, 1.0, 0.0).astype(BF16)
            flat = jnp.dot(q_parts[0], pick, preferred_element_type=F32)
            flat += jnp.dot(q_parts[1], pick, preferred_element_type=F32)
            q_row = jnp.zeros((mp, lanes), F32)
            for i in range(maxp):
                q_row += jnp.where(pos == float(i), flat[i * mp : (i + 1) * mp], 0.0)
            at = pos + lax.broadcasted_iota(jnp.int32, (nd, lanes), 0).astype(F32) - float(maxp - 1)
            entries = jnp.zeros((nd, lanes), F32)
            for j in range(maxp):
                entries += jnp.where(at == float(j), q_row[j : j + 1], 0.0)
            qd[:, aligned(c, lanes)] = jnp.where(at < count, entries, 0.0)
            return 0

        for c in range(p_size // 256):
            diagonals(c, 0)
            if c == 2:
                beta_copy(2).start()

    with jax.named_scope("trial_wait"):
        trial_copy.wait()
    psi_copy(0).start()

    mine_t = pl.ds(pl.multiple_of(bw + band * cols, cols), cols)

    def turn(k, _):
        own = trial_v[aligned(k, sw), :].T
        trial_t[:, aligned(k, sw)] = own
        lhs[mine_t, aligned(k, sw)] = own
        return 0

    with jax.named_scope("turn"):
        for k in range(g // sw):
            turn(k, 0)

    trial_x = pltpu.make_async_remote_copy(
        src_ref=trial_t,
        dst_ref=lhs.at[mine_t, :],
        send_sem=xs,
        recv_sem=xr,
        **partner,
    )

    def flip(to, first, k, rows):
        part = pl.ds(pl.multiple_of(first + k * rows, rows), rows)
        to[aligned(k, rows), :] = beta_v[:, part].T

    def project(c, _):
        with jax.named_scope("load"):
            beta_copy(c).wait()
        at = aligned(c, bw)
        with jax.named_scope("p1"):
            part = jnp.dot(trial_t[...], beta_v[:, at], preferred_element_type=F32)
            flip(lhs, 0, jnp.minimum(c, 1), bw // 2)
            code, scale = encode(part)
            proj[:, :, :, :, :, at] = part.reshape(2, 2, 2, 2, r1, bw)
            code1[:, :, :, :, :, at] = code.reshape(2, 2, 2, 2, r1, bw)
            scale1[c] = jnp.broadcast_to(scale, (1, 128))

        @pl.when(c == 0)
        def _():
            with jax.named_scope("barrier"):
                pl.semaphore_wait(barrier, len(met) + 1)
            trial_x.start()

        for i in range(beta_chunks):
            near = routes[i % 3][0]
            now = pl.ds(i * bw, bw)

            @pl.when(c == i)
            def _():
                for d in peers:
                    send(
                        code1.at[pick(near, d) + (slice(None), now)], scale1.at[i],
                        in1.at[d, :, :, :, now], in1s.at[i, d], recv1.at[i], device(near, d),
                    )
                for k in ((1,), (2, 3), ())[i]:
                    psi_copy(k).start()

        return 0

    lax.fori_loop(0, beta_chunks, project, 0)

    def keep(got, first, k):
        top, rest = split2(got)
        at = (aligned(first, bw), aligned(k, pw))
        g_hi[at] = top
        g_lo[at] = rest

    with jax.named_scope("trial_x"):
        trial_x.wait()

    def early(k, _):
        @pl.when(k == 2)
        def _():
            for c in range(beta_chunks):
                with jax.named_scope(f"mid1_{c}"):
                    middle1(c)

        with jax.named_scope("psi_wait"):
            psi_copy(k).wait()
        with jax.named_scope("bands_0"):
            at = aligned(k, pw)
            flip(beta_t, bw, k, 2 * bw // psi_chunks)
            got = jnp.dot(lhs[...], psi_v[:, at], preferred_element_type=F32)
            keep(got[:bw], 0, k)
            fin[..., at] = got[bw:].reshape(2, 2, 2, 2, r2, pw)
        return 0

    lax.fori_loop(0, psi_chunks, early, 0)

    plane, line = routes[0]

    def share_w(at, recv, to):
        a, b = wall.at[at], walls.at[at]
        send(a, b, a, b, recv, to)

    def block(d):
        return (band,) + cell(line, d) + cell(plane, 0)

    def weigh():
        with jax.named_scope("wait_z1"):
            for c in range(beta_chunks):
                landed(late1, recv1b.at[c])

        with jax.named_scope("q_apply"):
            pieces = []
            for c in range(beta_chunks):
                at = pl.ds(c * bw, bw)
                piece = mid1[cell(routes[c % 3][1], 0) + (slice(None), at)]
                for d in peers:
                    piece += decode(end1[d, :, at], end1s[c, d][:, :1])
                pieces.append(piece)
            x = jnp.concatenate(pieces, axis=1)
            acc = jnp.zeros_like(x)
            for d in range(2 * maxp - 1):
                shift = (maxp - 1 - d) % p_size
                moved = x if shift == 0 else pltpu.roll(x, shift, axis=1)
                acc += qd[d : d + 1, :] * moved
            code, scale = encode(acc)
            wall[(band,) + pick((3, 2), 0)[:2] + pick((1, 0), 0)[2:]] = code
            walls[(band,) + pick((3, 2), 0)[:2] + pick((1, 0), 0)[2:]] = jnp.broadcast_to(
                scale, (1, 128)
            )
        for d in peers:
            share_w(block(0), recv2.at[d - 1], device(line, d))
        for d in peers:
            share_w(block(0), recv2b.at[0], device(plane, d))

    def relay(e):
        landed(one, recv2.at[e - 1])
        for d in peers:
            share_w(block(e), recv2b.at[e], device(plane, d))

    def across(e):
        landed(3 * one, recv2b.at[e])
        row = (band,) + cell(line, e)
        a, b = wall.at[row], walls.at[row]
        send(a, b, a, b, recv2c.at[e], partner)

    def spread(b, e):
        high, low = cell(line, e)
        values = decode(wall[b, high, low], walls[b, high, low][..., :1])
        top, rest = split2(values.reshape(4 * r1, p_size))
        at = aligned(b * 4 + high * 2 + low, 4 * r1)
        w_hi[at, :] = top
        w_lo[at, :] = rest

    def late(u, _):
        for when, steps in (
            (1, (weigh,)),
            (3, (functools.partial(relay, 1),)),
            (4, (functools.partial(relay, 2),)),
            (5, (functools.partial(relay, 3), functools.partial(across, 0))),
            (6, (functools.partial(across, 1),)),
            (7, (functools.partial(across, 2),)),
        ):

            @pl.when(u == when)
            def _():
                with jax.named_scope(f"service_{when}"):
                    for step in steps:
                        step()

        with jax.named_scope("bands_1"):
            c, k = lax.div(u, psi_chunks), lax.rem(u, psi_chunks)
            rows = beta_t[aligned(c, bw), :]
            keep(jnp.dot(rows, psi_v[:, aligned(k, pw)], preferred_element_type=F32), c + 1, k)
        return 0

    lax.fori_loop(0, (beta_chunks - 1) * psi_chunks, late, 0)

    with jax.named_scope("ag_xy"):
        across(3)
    with jax.named_scope("spread_own"):
        for e in range(4):
            spread(band, e)
    with jax.named_scope("across"):
        for e in range(4):
            landed(4 * one, recv2c.at[e])
            spread(1 - band, e)

    def middle3(c):
        near, late = routes[c % 3]
        at = aligned(c, pw)
        landed(near3, recv3.at[c])
        total = fin[pick(near, 0) + (slice(None), at)].reshape(4 * r2, pw)
        for d in peers:
            total += decode(in3[d, :, :, :, at].reshape(4 * r2, pw), in3s[c, d][:, :1])
        code, scale = encode(total)
        scale3b[c] = jnp.broadcast_to(scale, (1, 128))
        code3b[:, :, :, at] = code.reshape(2, 2, r2, pw)
        mid3[:, :, :, at] = total.reshape(2, 2, r2, pw)
        for d in peers:
            send(
                code3b.at[cell(late, d) + (slice(None), at)], scale3b.at[c],
                end3.at[d, :, at], end3s.at[c, d], recv3b.at[c], device(late, d),
            )

    def product(c):
        at = aligned(c, pw)
        f = jnp.dot(w_hi[...], g_hi[:, at], preferred_element_type=F32)
        f += jnp.dot(w_hi[...], g_lo[:, at], preferred_element_type=F32)
        f += jnp.dot(w_lo[...], g_hi[:, at], preferred_element_type=F32)
        return f + fin[..., at].reshape(2 * cols, pw)

    def share(c, f):
        near = routes[c % 3][0]
        at = aligned(c, pw)
        code, scale = encode(f)
        scale3[c] = jnp.broadcast_to(scale, (1, 128))
        code3[..., at] = code.reshape(2, 2, 2, 2, r2, pw)
        fin[..., at] = f.reshape(2, 2, 2, 2, r2, pw)
        for d in peers:
            send(
                code3.at[pick(near, d) + (slice(None), at)], scale3.at[c],
                in3.at[d, :, :, :, at], in3s.at[c, d], recv3.at[c], device(near, d),
            )

    with jax.named_scope("share"):
        f = product(0)
        for c in range(psi_chunks):
            later = product(c + 1) if c + 1 < psi_chunks else None
            share(c, f)
            f = later
    for c in range(psi_chunks):
        with jax.named_scope(f"mid3_{c}"):
            middle3(c)

    with jax.named_scope("tail"):
        for c in range(psi_chunks):
            at = aligned(c, pw)
            landed(late3, recv3b.at[c])
            total = mid3[cell(routes[c % 3][1], 0) + (slice(None), at)]
            for d in peers:
                total += decode(end3[d, :, at], end3s[c, d][:, :1])
            out_ref[:, at] = total

    with jax.named_scope("drain"):
        total = beta_chunks * (near1 + late1) + psi_chunks * (near3 + late3) + 31 * one
        counted(total, recv1.at[0]).wait_send()


def fused(n, blk, psi, trial, beta, q_blocks, atom_counts):
    g, cols = trial.shape
    nbands = psi.shape[1]
    p_size = beta.shape[1]
    natom, maxp = q_blocks.shape[:2]
    mp = -(-maxp // 8) * 8
    nd = -(-(2 * maxp - 1) // 8) * 8
    r1, r2 = cols // n, blk // n
    bc, pc = 3, 4
    meter = (2 * (15 * (cols * p_size + blk * nbands) // 16) + 2 * 16 * cols * p_size) // 512 + 256
    dma = pltpu.SemaphoreType.DMA
    vm = pltpu.VMEM
    out = pl.pallas_call(
        functools.partial(kernel, n, maxp),
        out_shape=jax.ShapeDtypeStruct((r2, nbands), F32),
        in_specs=[pl.BlockSpec(memory_space=pl.ANY)] * 5,
        out_specs=pl.BlockSpec(memory_space=pltpu.VMEM),
        scratch_shapes=[
            vm((g, nbands), BF16),
            vm((g, p_size), BF16),
            vm((g, cols), BF16),
            vm((maxp, maxp, natom), F32),
            vm((1, natom), jnp.int32),
            vm((p_size // bc + blk, g), BF16),
            vm((p_size - p_size // bc, g), BF16),
            vm((cols, g), BF16),
            vm((2, maxp * mp, natom), BF16),
            vm((nd, p_size), F32),
            vm((p_size, nbands), BF16),
            vm((p_size, nbands), BF16),
            vm((blk, p_size), BF16),
            vm((blk, p_size), BF16),
            vm((2, 2, 2, 2, r1, p_size), F32),
            vm((2, 2, 2, 2, r1, p_size), I16),
            vm((bc, 1, 128), F32),
            vm((4, 2, 2, r1, p_size), I16),
            vm((bc, 4, 1, 128), F32),
            vm((2, 2, r1, p_size), F32),
            vm((2, 2, r1, p_size), I16),
            vm((bc, 1, 128), F32),
            vm((4, r1, p_size), I16),
            vm((bc, 4, 1, 128), F32),
            vm((2, 2, 2, 2, 2, r1, p_size), I16),
            vm((2, 2, 2, 2, 2, 1, 128), F32),
            vm((2, 2, 2, 2, r2, nbands), F32),
            vm((2, 2, 2, 2, r2, nbands), I16),
            vm((pc, 1, 128), F32),
            vm((4, 2, 2, r2, nbands), I16),
            vm((pc, 4, 1, 128), F32),
            vm((2, 2, r2, nbands), F32),
            vm((2, 2, r2, nbands), I16),
            vm((pc, 1, 128), F32),
            vm((4, r2, nbands), I16),
            vm((pc, 4, 1, 128), F32),
            vm((meter, 1, 128), F32),
            dma((2,)),
            dma,
            dma((bc,)),
            dma((pc,)),
            dma,
            dma,
            dma,
            dma((bc,)),
            dma((bc,)),
            dma((3,)),
            dma((4,)),
            dma((4,)),
            dma((pc,)),
            dma((pc,)),
        ],
        compiler_params=pltpu.CompilerParams(
            collective_id=0, has_side_effects=True, vmem_limit_bytes=62 * 1024 * 1024
        ),
    )(psi, trial, beta, q_blocks.transpose(1, 2, 0), atom_counts.reshape(1, natom))
    return out.T


def q_dense(atom_counts, q_blocks, p_size):
    offsets = jnp.cumsum(atom_counts, dtype=jnp.int32) - atom_counts
    natom, maxp = q_blocks.shape[:2]
    ids = jnp.arange(p_size, dtype=jnp.int32)
    owns = (offsets[None, :] <= ids[:, None]) & (ids[:, None] < (offsets + atom_counts)[None, :])
    pos = jnp.sum(jnp.where(owns, ids[:, None] - offsets[None, :], 0), axis=1)
    atom = jnp.sum(jnp.where(owns, jnp.arange(natom, dtype=jnp.int32)[None, :], 0), axis=1)
    flat = jnp.dot(owns.astype(F32), q_blocks.reshape(natom, maxp * maxp), precision=precise)
    place = pos[:, None] == jnp.arange(maxp, dtype=jnp.int32)[None, :]
    rows = jnp.sum(jnp.where(place[:, :, None], flat.reshape(p_size, maxp, maxp), 0.0), axis=1)
    entries = jnp.dot(rows, place.astype(F32).T, precision=precise)
    return jnp.where(atom[:, None] == atom[None, :], entries, 0.0)


def general(psi, trial, beta, q_blocks, atom_counts):
    own = lax.psum(contract(beta, trial), "ga")
    weighted = jnp.dot(q_dense(atom_counts, q_blocks, beta.shape[1]), own, precision=precise)
    w_hi, w_lo = split2(weighted)
    both = jnp.dot(beta, jnp.concatenate([w_hi, w_lo], axis=1), preferred_element_type=F32)
    cols = trial.shape[1]
    s = both[:, :cols] + both[:, cols:] + trial.astype(F32)
    s_hi, s_lo = split2(lax.all_gather(s, "band", axis=1, tiled=True))
    part = contract(psi, s_hi) + contract(psi, s_lo)
    return lax.psum_scatter(part, "ga", scatter_dimension=1, tiled=True)


def solution(mesh):
    n, bands = mesh.shape["ga"], mesh.shape["band"]

    def shards(psi, trial, beta, q_blocks, atom_counts):
        g, cols = trial.shape
        blk = cols * bands
        fits = (
            bands == 2
            and n == 16
            and cols % 128 == 0
            and cols % (8 * n) == 0
            and blk % (8 * n) == 0
            and g % 4096 == 0
            and beta.shape[1] % 768 == 0
            and psi.shape[1] % 512 == 0
            and q_blocks.shape[0] % 128 == 0
        )
        if fits:
            return fused(n, blk, psi, trial, beta, q_blocks, atom_counts)
        return general(psi, trial, beta, q_blocks, atom_counts)

    in_specs = (P("ga", "band"), P("ga", "band"), P("ga", None), P(), P())
    out_specs = P("band", "ga")
    return jax.shard_map(shards, mesh=mesh, in_specs=in_specs, out_specs=out_specs, check_vma=False)
```

```python
import functools

import jax
import jax.numpy as jnp
from jax import lax
from jax.experimental import pallas as pl
from jax.experimental.pallas import tpu as pltpu
from jax.sharding import PartitionSpec as P

MESH = pl.DeviceIdType.MESH
precise = lax.Precision.HIGHEST
F32, BF16, I16 = jnp.float32, jnp.bfloat16, jnp.int16
LEVELS, TINY = 32767.0, 1e-30


def contract(left, right, precision=None):
    return lax.dot_general(
        left, right, (((0,), (0,)), ((), ())), precision=precision, preferred_element_type=F32
    )


def split2(x):
    hi = x.astype(BF16)
    return hi, (x - hi.astype(F32)).astype(BF16)


def encode(x, top=None):
    if top is None:
        top = jnp.max(jnp.abs(x), axis=0, keepdims=True)
    top = jnp.maximum(top, TINY)
    return jnp.round(x * (LEVELS / top)).astype(jnp.int32).astype(I16), top * (1.0 / LEVELS)


def decode(code, scale):
    return code.astype(jnp.int32).astype(F32) * scale


def kernel(
    n, maxp, psi_h, trial_h, beta_h, q_h, cnt_h, out_ref,
    psi_v, beta_v, trial_v, q_v, cnt_v, lhs, beta_t, trial_t, q_parts, qd, g_hi, g_lo, w_hi, w_lo,
    proj, code1, scale1, in1, in1s, mid1, code1b, scale1b, end1, end1s,
    wall, walls, fin, code3, scale3, in3, in3s, mid3, code3b, scale3b, end3, end3s, meter,
    q_sem, trial_sem, beta_sem, psi_sem, xs, xr, sent, recv1, recv1b, recv2, recv2b, recv2c,
    recv3, recv3b,
):
    me = lax.axis_index("ga")
    band = lax.axis_index("band")
    bit = [lax.rem(lax.div(me, 1 << p), 2) for p in range(4)]
    routes = (((1, 0), (3, 2)), ((2, 1), (3, 0)), ((2, 0), (3, 1)))
    peers = (3, 2, 1)

    def toggled(pair, d):
        return {p: lax.rem(bit[p] + (d >> k & 1), 2) for k, p in enumerate(pair[::-1])}

    def device(pair, d):
        there = sum((v - bit[p]) * (1 << p) for p, v in toggled(pair, d).items())
        return dict(device_id=(me + there, band), device_id_type=MESH)

    def pick(pair, d):
        bits = toggled(pair, d)
        return tuple(bits.get(p, slice(None)) for p in (3, 2, 1, 0))

    def cell(pair, d):
        bits = toggled(pair, d)
        return tuple(bits[p] for p in pair)

    partner = dict(device_id=(me, 1 - band), device_id_type=MESH)

    g, cols = trial_v.shape
    p_size = beta_v.shape[1]
    nbands = psi_v.shape[1]
    natom = cnt_v.shape[1]
    mp = q_parts.shape[1] // maxp
    r1 = cols // n
    r2 = out_ref.shape[0]
    beta_chunks = beta_sem.shape[0]
    bw = p_size // beta_chunks
    psi_chunks = psi_sem.shape[0]
    pw = nbands // psi_chunks
    sw = 512

    def aligned(i, size):
        return pl.ds(i * size if isinstance(i, int) else pl.multiple_of(i * size, size), size)

    def beta_copy(c):
        at = (slice(None), pl.ds(c * bw, bw))
        return pltpu.make_async_copy(beta_h.at[at], beta_v.at[at], beta_sem.at[c])

    def psi_copy(c):
        at = (slice(None), pl.ds(c * pw, pw))
        return pltpu.make_async_copy(psi_h.at[at], psi_v.at[at], psi_sem.at[c])

    q_copy = pltpu.make_async_copy(q_h, q_v, q_sem.at[0])
    cnt_copy = pltpu.make_async_copy(cnt_h, cnt_v, q_sem.at[1])
    trial_copy = pltpu.make_async_copy(trial_h, trial_v, trial_sem)
    q_copy.start()
    cnt_copy.start()
    trial_copy.start()
    beta_copy(0).start()

    barrier = pltpu.get_barrier_semaphore()

    met = [(pair, d) for pair in routes[0] for d in peers]
    met += [(pair, 3) for route in routes[1:] for pair in route]
    for pair, d in met:
        pl.semaphore_signal(barrier, inc=1, **device(pair, d))
    pl.semaphore_signal(barrier, inc=1, **partner)

    def send(src, src_s, dst, dst_s, recv, to):
        for a, b in ((src, dst), (src_s, dst_s)):
            pltpu.make_async_remote_copy(
                src_ref=a, dst_ref=b, send_sem=sent, recv_sem=recv, **to
            ).start()

    def size(values, lanes, copies):
        return copies * (2 * values + 4 * lanes) // (4 * 128)

    def counted(rows, recv):
        a = meter.at[pl.ds(0, rows)]
        return pltpu.make_async_remote_copy(
            src_ref=a, dst_ref=a, send_sem=sent, recv_sem=recv, **partner
        )

    def landed(rows, recv):
        counted(rows, recv).wait_recv()

    near1, late1 = size(4 * r1 * bw, bw, 3), size(r1 * bw, bw, 3)
    near3, late3 = size(4 * r2 * pw, pw, 3), size(r2 * pw, pw, 3)
    one = size(r1 * p_size, 128, 1)

    def middle1(c):
        near, late = routes[c % 3]
        at = pl.ds(c * bw, bw)
        landed(near1, recv1.at[c])
        total = proj[pick(near, 0) + (slice(None), at)].reshape(4 * r1, bw)
        for d in peers:
            total += decode(in1[d, :, :, :, at].reshape(4 * r1, bw), in1s[c, d])
        code, scale = encode(total)
        scale1b[c] = scale
        code1b[:, :, :, at] = code.reshape(2, 2, r1, bw)
        mid1[:, :, :, at] = total.reshape(2, 2, r1, bw)
        for d in peers:
            send(
                code1b.at[cell(late, d) + (slice(None), at)], scale1b.at[c],
                end1.at[d, :, at], end1s.at[c, d], recv1b.at[c], device(late, d),
            )

    with jax.named_scope("q_wait"):
        q_copy.wait()
        cnt_copy.wait()
    beta_copy(1).start()
    with jax.named_scope("diag"):
        cnt = cnt_v[...].astype(F32)
        row = lax.broadcasted_iota(jnp.int32, (natom, natom), 0)
        col = lax.broadcasted_iota(jnp.int32, (natom, natom), 1)
        offs = jnp.sum(jnp.where(col < row, cnt, 0.0), axis=1, keepdims=True)
        own = jnp.sum(jnp.where(col == row, cnt, 0.0), axis=1, keepdims=True)
        q_parts[...] = jnp.zeros_like(q_parts)
        for i in range(maxp):
            q = q_v[i]
            q_hi = q.astype(BF16)
            at = slice(i * mp, i * mp + maxp)
            q_parts[0, at] = q_hi
            q_parts[1, at] = (q - q_hi.astype(F32)).astype(BF16)

        def diagonals(c, _):
            lanes = 256
            nd = qd.shape[0]
            ids = (c * lanes + lax.broadcasted_iota(jnp.int32, (natom, lanes), 1)).astype(F32)
            owns = (offs <= ids) & (ids < offs + own)
            pos = jnp.sum(jnp.where(owns, ids - offs, 0.0), axis=0, keepdims=True)
            count = jnp.sum(
                jnp.where(owns, jnp.broadcast_to(own, owns.shape), 0.0), axis=0, keepdims=True
            )
            pick = jnp.where(owns, 1.0, 0.0).astype(BF16)
            flat = jnp.dot(q_parts[0], pick, preferred_element_type=F32)
            flat += jnp.dot(q_parts[1], pick, preferred_element_type=F32)
            q_row = jnp.zeros((mp, lanes), F32)
            for i in range(maxp):
                q_row = jnp.where(pos == float(i), flat[i * mp : (i + 1) * mp], q_row)
            at = pos + lax.broadcasted_iota(jnp.int32, (nd, lanes), 0).astype(F32) - float(maxp - 1)
            entries = jnp.zeros((nd, lanes), F32)
            for j in range(maxp):
                entries = jnp.where(at == float(j), q_row[j : j + 1], entries)
            qd[:, aligned(c, lanes)] = jnp.where(at < count, entries, 0.0)
            return 0

        for c in range(p_size // 256):
            diagonals(c, 0)
            if c == 2:
                beta_copy(2).start()

    with jax.named_scope("trial_wait"):
        trial_copy.wait()
    psi_copy(0).start()

    mine_t = pl.ds(pl.multiple_of(bw + band * cols, cols), cols)

    def turn(k, _):
        own = trial_v[aligned(k, sw), :].T
        trial_t[:, aligned(k, sw)] = own
        lhs[mine_t, aligned(k, sw)] = own
        return 0

    with jax.named_scope("turn"):
        for k in range(g // sw):
            turn(k, 0)

    trial_x = pltpu.make_async_remote_copy(
        src_ref=trial_t,
        dst_ref=lhs.at[mine_t, :],
        send_sem=xs,
        recv_sem=xr,
        **partner,
    )

    def flip(to, first, k, rows):
        part = pl.ds(pl.multiple_of(first + k * rows, rows), rows)
        to[aligned(k, rows), :] = beta_v[:, part].T

    def project(c, _):
        with jax.named_scope("load"):
            beta_copy(c).wait()
        at = aligned(c, bw)
        with jax.named_scope("p1"):
            part = jnp.dot(trial_t[...], beta_v[:, at], preferred_element_type=F32)
            flip(lhs, 0, jnp.minimum(c, 1), bw // 2)
            code, scale = encode(part)
            proj[:, :, :, :, :, at] = part.reshape(2, 2, 2, 2, r1, bw)
            code1[:, :, :, :, :, at] = code.reshape(2, 2, 2, 2, r1, bw)
            scale1[c] = scale

        @pl.when(c == 0)
        def _():
            with jax.named_scope("barrier"):
                pl.semaphore_wait(barrier, len(met) + 1)
            trial_x.start()

        for i in range(beta_chunks):
            near = routes[i % 3][0]
            now = pl.ds(i * bw, bw)

            @pl.when(c == i)
            def _():
                for d in peers:
                    send(
                        code1.at[pick(near, d) + (slice(None), now)], scale1.at[i],
                        in1.at[d, :, :, :, now], in1s.at[i, d], recv1.at[i], device(near, d),
                    )
                for k in ((1,), (2, 3), ())[i]:
                    psi_copy(k).start()

        return 0

    lax.fori_loop(0, beta_chunks, project, 0)

    def keep(got, first, k):
        top, rest = split2(got)
        at = (aligned(first, bw), aligned(k, pw))
        g_hi[at] = top
        g_lo[at] = rest

    with jax.named_scope("trial_x"):
        trial_x.wait()

    def early(k, _):
        @pl.when(k == 2)
        def _():
            for c in range(beta_chunks):
                with jax.named_scope(f"mid1_{c}"):
                    middle1(c)

        with jax.named_scope("psi_wait"):
            psi_copy(k).wait()
        with jax.named_scope("bands_0"):
            at = aligned(k, pw)
            flip(beta_t, bw, k, 2 * bw // psi_chunks)
            got = jnp.dot(lhs[...], psi_v[:, at], preferred_element_type=F32)
            keep(got[:bw], 0, k)
            fin[..., at] = got[bw:].reshape(2, 2, 2, 2, r2, pw)
        return 0

    lax.fori_loop(0, psi_chunks, early, 0)

    plane, line = routes[0]

    def share_w(at, recv, to):
        a, b = wall.at[at], walls.at[at]
        send(a, b, a, b, recv, to)

    def block(d):
        return (band,) + cell(line, d) + cell(plane, 0)

    def weigh():
        with jax.named_scope("wait_z1"):
            for c in range(beta_chunks):
                landed(late1, recv1b.at[c])

        with jax.named_scope("q_apply"):
            pieces = []
            for c in range(beta_chunks):
                at = pl.ds(c * bw, bw)
                piece = mid1[cell(routes[c % 3][1], 0) + (slice(None), at)]
                for d in peers:
                    piece += decode(end1[d, :, at], end1s[c, d])
                pieces.append(piece)
            x = jnp.concatenate(pieces, axis=1)
            acc = jnp.zeros_like(x)
            for d in range(2 * maxp - 1):
                shift = (maxp - 1 - d) % p_size
                moved = x if shift == 0 else pltpu.roll(x, shift, axis=1)
                acc += qd[d : d + 1, :] * moved
            tiles = [acc[:, t : t + 128] for t in range(0, p_size, 128)]
            top = functools.reduce(jnp.maximum, [jnp.abs(t) for t in tiles])
            top = jnp.max(top, axis=0, keepdims=True)
            code, scale = encode(acc, jnp.concatenate([top] * len(tiles), axis=1))
            wall[(band,) + pick((3, 2), 0)[:2] + pick((1, 0), 0)[2:]] = code
            walls[(band,) + pick((3, 2), 0)[:2] + pick((1, 0), 0)[2:]] = scale[:, :128]
        for d in peers:
            share_w(block(0), recv2.at[d - 1], device(line, d))
        for d in peers:
            share_w(block(0), recv2b.at[0], device(plane, d))

    def relay(e):
        landed(one, recv2.at[e - 1])
        for d in peers:
            share_w(block(e), recv2b.at[e], device(plane, d))

    def across(e):
        landed(3 * one, recv2b.at[e])
        row = (band,) + cell(line, e)
        a, b = wall.at[row], walls.at[row]
        send(a, b, a, b, recv2c.at[e], partner)

    def spread(b, e):
        high, low = cell(line, e)
        scale = jnp.concatenate([walls[b, high, low]] * (p_size // 128), axis=-1)
        values = decode(wall[b, high, low], scale)
        top, rest = split2(values.reshape(4 * r1, p_size))
        at = aligned(b * 4 + high * 2 + low, 4 * r1)
        w_hi[at, :] = top
        w_lo[at, :] = rest

    def late(u, _):
        for when, steps in (
            (1, (weigh,)),
            (3, (functools.partial(relay, 1),)),
            (4, (functools.partial(relay, 2),)),
            (5, (functools.partial(relay, 3), functools.partial(across, 0))),
            (6, (functools.partial(across, 1),)),
            (7, (functools.partial(across, 2),)),
        ):

            @pl.when(u == when)
            def _():
                with jax.named_scope(f"service_{when}"):
                    for step in steps:
                        step()

        with jax.named_scope("bands_1"):
            c, k = lax.div(u, psi_chunks), lax.rem(u, psi_chunks)
            rows = beta_t[aligned(c, bw), :]
            keep(jnp.dot(rows, psi_v[:, aligned(k, pw)], preferred_element_type=F32), c + 1, k)
        return 0

    lax.fori_loop(0, (beta_chunks - 1) * psi_chunks, late, 0)

    with jax.named_scope("ag_xy"):
        across(3)
    with jax.named_scope("spread_own"):
        for e in range(4):
            spread(band, e)
    with jax.named_scope("across"):
        for e in range(4):
            landed(4 * one, recv2c.at[e])
            spread(1 - band, e)

    def middle3(c):
        near, late = routes[c % 3]
        at = aligned(c, pw)
        landed(near3, recv3.at[c])
        total = fin[pick(near, 0) + (slice(None), at)].reshape(4 * r2, pw)
        for d in peers:
            total += decode(in3[d, :, :, :, at].reshape(4 * r2, pw), in3s[c, d])
        code, scale = encode(total)
        scale3b[c] = scale
        code3b[:, :, :, at] = code.reshape(2, 2, r2, pw)
        mid3[:, :, :, at] = total.reshape(2, 2, r2, pw)
        for d in peers:
            send(
                code3b.at[cell(late, d) + (slice(None), at)], scale3b.at[c],
                end3.at[d, :, at], end3s.at[c, d], recv3b.at[c], device(late, d),
            )

    def product(c):
        at = aligned(c, pw)
        f = jnp.dot(w_hi[...], g_hi[:, at], preferred_element_type=F32)
        f += jnp.dot(w_hi[...], g_lo[:, at], preferred_element_type=F32)
        f += jnp.dot(w_lo[...], g_hi[:, at], preferred_element_type=F32)
        return f + fin[..., at].reshape(2 * cols, pw)

    def share(c, f):
        near = routes[c % 3][0]
        at = aligned(c, pw)
        code, scale = encode(f)
        scale3[c] = scale
        code3[..., at] = code.reshape(2, 2, 2, 2, r2, pw)
        fin[..., at] = f.reshape(2, 2, 2, 2, r2, pw)
        for d in peers:
            send(
                code3.at[pick(near, d) + (slice(None), at)], scale3.at[c],
                in3.at[d, :, :, :, at], in3s.at[c, d], recv3.at[c], device(near, d),
            )

    with jax.named_scope("share"):
        f = product(0)
        for c in range(psi_chunks):
            later = product(c + 1) if c + 1 < psi_chunks else None
            share(c, f)
            f = later
    for c in range(psi_chunks):
        with jax.named_scope(f"mid3_{c}"):
            middle3(c)

    with jax.named_scope("tail"):
        for c in range(psi_chunks):
            at = aligned(c, pw)
            landed(late3, recv3b.at[c])
            total = mid3[cell(routes[c % 3][1], 0) + (slice(None), at)]
            for d in peers:
                total += decode(end3[d, :, at], end3s[c, d])
            out_ref[:, at] = total

    with jax.named_scope("drain"):
        total = beta_chunks * (near1 + late1) + psi_chunks * (near3 + late3) + 31 * one
        counted(total, recv1.at[0]).wait_send()


def fused(n, blk, psi, trial, beta, q_blocks, atom_counts):
    g, cols = trial.shape
    nbands = psi.shape[1]
    p_size = beta.shape[1]
    natom, maxp = q_blocks.shape[:2]
    mp = -(-maxp // 8) * 8
    nd = -(-(2 * maxp - 1) // 8) * 8
    r1, r2 = cols // n, blk // n
    bc, pc = 3, 4
    meter = (2 * (15 * (cols * p_size + blk * nbands) // 16) + 2 * 16 * cols * p_size) // 512 + 1024
    dma = pltpu.SemaphoreType.DMA
    vm = pltpu.VMEM
    out = pl.pallas_call(
        functools.partial(kernel, n, maxp),
        out_shape=jax.ShapeDtypeStruct((r2, nbands), F32),
        in_specs=[pl.BlockSpec(memory_space=pl.ANY)] * 5,
        out_specs=pl.BlockSpec(memory_space=pltpu.VMEM),
        scratch_shapes=[
            vm((g, nbands), BF16),
            vm((g, p_size), BF16),
            vm((g, cols), BF16),
            vm((maxp, maxp, natom), F32),
            vm((1, natom), jnp.int32),
            vm((p_size // bc + blk, g), BF16),
            vm((p_size - p_size // bc, g), BF16),
            vm((cols, g), BF16),
            vm((2, maxp * mp, natom), BF16),
            vm((nd, p_size), F32),
            vm((p_size, nbands), BF16),
            vm((p_size, nbands), BF16),
            vm((blk, p_size), BF16),
            vm((blk, p_size), BF16),
            vm((2, 2, 2, 2, r1, p_size), F32),
            vm((2, 2, 2, 2, r1, p_size), I16),
            vm((bc, 1, p_size // bc), F32),
            vm((4, 2, 2, r1, p_size), I16),
            vm((bc, 4, 1, p_size // bc), F32),
            vm((2, 2, r1, p_size), F32),
            vm((2, 2, r1, p_size), I16),
            vm((bc, 1, p_size // bc), F32),
            vm((4, r1, p_size), I16),
            vm((bc, 4, 1, p_size // bc), F32),
            vm((2, 2, 2, 2, 2, r1, p_size), I16),
            vm((2, 2, 2, 2, 2, 1, 128), F32),
            vm((2, 2, 2, 2, r2, nbands), F32),
            vm((2, 2, 2, 2, r2, nbands), I16),
            vm((pc, 1, nbands // pc), F32),
            vm((4, 2, 2, r2, nbands), I16),
            vm((pc, 4, 1, nbands // pc), F32),
            vm((2, 2, r2, nbands), F32),
            vm((2, 2, r2, nbands), I16),
            vm((pc, 1, nbands // pc), F32),
            vm((4, r2, nbands), I16),
            vm((pc, 4, 1, nbands // pc), F32),
            vm((meter, 1, 128), F32),
            dma((2,)),
            dma,
            dma((bc,)),
            dma((pc,)),
            dma,
            dma,
            dma,
            dma((bc,)),
            dma((bc,)),
            dma((3,)),
            dma((4,)),
            dma((4,)),
            dma((pc,)),
            dma((pc,)),
        ],
        compiler_params=pltpu.CompilerParams(
            collective_id=0, has_side_effects=True, vmem_limit_bytes=62 * 1024 * 1024
        ),
    )(psi, trial, beta, q_blocks.transpose(1, 2, 0), atom_counts.reshape(1, natom))
    return out.T


def q_dense(atom_counts, q_blocks, p_size):
    offsets = jnp.cumsum(atom_counts, dtype=jnp.int32) - atom_counts
    natom, maxp = q_blocks.shape[:2]
    ids = jnp.arange(p_size, dtype=jnp.int32)
    owns = (offsets[None, :] <= ids[:, None]) & (ids[:, None] < (offsets + atom_counts)[None, :])
    pos = jnp.sum(jnp.where(owns, ids[:, None] - offsets[None, :], 0), axis=1)
    atom = jnp.sum(jnp.where(owns, jnp.arange(natom, dtype=jnp.int32)[None, :], 0), axis=1)
    flat = jnp.dot(owns.astype(F32), q_blocks.reshape(natom, maxp * maxp), precision=precise)
    place = pos[:, None] == jnp.arange(maxp, dtype=jnp.int32)[None, :]
    rows = jnp.sum(jnp.where(place[:, :, None], flat.reshape(p_size, maxp, maxp), 0.0), axis=1)
    entries = jnp.dot(rows, place.astype(F32).T, precision=precise)
    return jnp.where(atom[:, None] == atom[None, :], entries, 0.0)


def general(psi, trial, beta, q_blocks, atom_counts):
    own = lax.psum(contract(beta, trial), "ga")
    weighted = jnp.dot(q_dense(atom_counts, q_blocks, beta.shape[1]), own, precision=precise)
    w_hi, w_lo = split2(weighted)
    both = jnp.dot(beta, jnp.concatenate([w_hi, w_lo], axis=1), preferred_element_type=F32)
    cols = trial.shape[1]
    s = both[:, :cols] + both[:, cols:] + trial.astype(F32)
    s_hi, s_lo = split2(lax.all_gather(s, "band", axis=1, tiled=True))
    part = contract(psi, s_hi) + contract(psi, s_lo)
    return lax.psum_scatter(part, "ga", scatter_dimension=1, tiled=True)


def solution(mesh):
    n, bands = mesh.shape["ga"], mesh.shape["band"]

    def shards(psi, trial, beta, q_blocks, atom_counts):
        g, cols = trial.shape
        blk = cols * bands
        fits = (
            bands == 2
            and n == 16
            and cols % 128 == 0
            and cols % (8 * n) == 0
            and blk % (8 * n) == 0
            and g % 4096 == 0
            and beta.shape[1] % 768 == 0
            and psi.shape[1] % 512 == 0
            and q_blocks.shape[0] % 128 == 0
        )
        if fits:
            return fused(n, blk, psi, trial, beta, q_blocks, atom_counts)
        return general(psi, trial, beta, q_blocks, atom_counts)

    in_specs = (P("ga", "band"), P("ga", "band"), P("ga", None), P(), P())
    out_specs = P("band", "ga")
    return jax.shard_map(shards, mesh=mesh, in_specs=in_specs, out_specs=out_specs, check_vma=False)
```

```python
import functools

import jax
import jax.numpy as jnp
from jax import lax
from jax.experimental import pallas as pl
from jax.experimental.pallas import tpu as pltpu
from jax.sharding import PartitionSpec as P

MESH = pl.DeviceIdType.MESH
precise = lax.Precision.HIGHEST
F32, BF16, I16 = jnp.float32, jnp.bfloat16, jnp.int16
LEVELS, TINY = 32767.0, 1e-30


def contract(left, right, precision=None):
    return lax.dot_general(
        left, right, (((0,), (0,)), ((), ())), precision=precision, preferred_element_type=F32
    )


def split2(x):
    hi = x.astype(BF16)
    return hi, (x - hi.astype(F32)).astype(BF16)


def encode(x, top=None):
    if top is None:
        top = jnp.max(jnp.abs(x), axis=0, keepdims=True)
    top = jnp.maximum(top, TINY)
    return jnp.round(x * (LEVELS / top)).astype(jnp.int32).astype(I16), top * (1.0 / LEVELS)


def decode(code, scale):
    return code.astype(jnp.int32).astype(F32) * scale


def kernel(
    n, maxp, psi_h, trial_h, beta_h, q_h, cnt_h, out_ref,
    psi_v, beta_v, trial_v, q_v, cnt_v, lhs, beta_t, trial_t, q_parts, qd, g_hi, g_lo, w_hi, w_lo,
    proj, code1, scale1, in1, in1s, mid1, code1b, scale1b, end1, end1s,
    wall, walls, fin, code3, scale3, in3, in3s, mid3, code3b, scale3b, end3, end3s, meter,
    q_sem, trial_sem, beta_sem, psi_sem, xs, xr, sent, recv1, recv1b, recv2, recv2b, recv2c,
    recv3, recv3b,
):
    me = lax.axis_index("ga")
    band = lax.axis_index("band")
    bit = [lax.rem(lax.div(me, 1 << p), 2) for p in range(4)]
    routes = (((1, 0), (3, 2)), ((2, 1), (3, 0)), ((2, 0), (3, 1)))
    peers = (3, 2, 1)

    def toggled(pair, d):
        return {p: lax.rem(bit[p] + (d >> k & 1), 2) for k, p in enumerate(pair[::-1])}

    def device(pair, d):
        there = sum((v - bit[p]) * (1 << p) for p, v in toggled(pair, d).items())
        return dict(device_id=(me + there, band), device_id_type=MESH)

    def pick(pair, d):
        bits = toggled(pair, d)
        return tuple(bits.get(p, slice(None)) for p in (3, 2, 1, 0))

    def cell(pair, d):
        bits = toggled(pair, d)
        return tuple(bits[p] for p in pair)

    partner = dict(device_id=(me, 1 - band), device_id_type=MESH)

    g, cols = trial_v.shape
    p_size = beta_v.shape[1]
    nbands = psi_v.shape[1]
    natom = cnt_v.shape[1]
    mp = q_parts.shape[1] // maxp
    r1 = cols // n
    r2 = out_ref.shape[0]
    beta_chunks = beta_sem.shape[0]
    bw = p_size // beta_chunks
    psi_chunks = psi_sem.shape[0]
    pw = nbands // psi_chunks
    sw = 512

    def aligned(i, size):
        return pl.ds(i * size if isinstance(i, int) else pl.multiple_of(i * size, size), size)

    def beta_copy(c):
        at = (slice(None), pl.ds(c * bw, bw))
        return pltpu.make_async_copy(beta_h.at[at], beta_v.at[at], beta_sem.at[c])

    def psi_copy(c):
        at = (slice(None), pl.ds(c * pw, pw))
        return pltpu.make_async_copy(psi_h.at[at], psi_v.at[at], psi_sem.at[c])

    q_copy = pltpu.make_async_copy(q_h, q_v, q_sem.at[0])
    cnt_copy = pltpu.make_async_copy(cnt_h, cnt_v, q_sem.at[1])
    trial_copy = pltpu.make_async_copy(trial_h, trial_v, trial_sem)
    q_copy.start()
    cnt_copy.start()
    trial_copy.start()
    beta_copy(0).start()

    barrier = pltpu.get_barrier_semaphore()

    met = [(pair, d) for pair in routes[0] for d in peers]
    met += [(pair, 3) for route in routes[1:] for pair in route]
    for pair, d in met:
        pl.semaphore_signal(barrier, inc=1, **device(pair, d))
    pl.semaphore_signal(barrier, inc=1, **partner)

    def send(src, src_s, dst, dst_s, recv, to):
        for a, b in ((src, dst), (src_s, dst_s)):
            pltpu.make_async_remote_copy(
                src_ref=a, dst_ref=b, send_sem=sent, recv_sem=recv, **to
            ).start()

    def size(values, lanes, copies):
        return copies * (2 * values + 4 * lanes) // (4 * 128)

    def counted(rows, recv):
        a = meter.at[pl.ds(0, rows)]
        return pltpu.make_async_remote_copy(
            src_ref=a, dst_ref=a, send_sem=sent, recv_sem=recv, **partner
        )

    def landed(rows, recv):
        counted(rows, recv).wait_recv()

    near1, late1 = size(4 * r1 * bw, bw, 3), size(r1 * bw, bw, 3)
    near3, late3 = size(4 * r2 * pw, pw, 3), size(r2 * pw, pw, 3)
    one = size(r1 * p_size, 128, 1)

    def middle1(c):
        near, late = routes[c % 3]
        at = pl.ds(c * bw, bw)
        landed(near1, recv1.at[c])
        total = proj[pick(near, 0) + (slice(None), at)].reshape(4 * r1, bw)
        for d in peers:
            total += decode(in1[d, :, :, :, at].reshape(4 * r1, bw), in1s[c, d])
        code, scale = encode(total)
        scale1b[c] = scale
        code1b[:, :, :, at] = code.reshape(2, 2, r1, bw)
        mid1[:, :, :, at] = total.reshape(2, 2, r1, bw)
        for d in peers:
            send(
                code1b.at[cell(late, d) + (slice(None), at)], scale1b.at[c],
                end1.at[d, :, at], end1s.at[c, d], recv1b.at[c], device(late, d),
            )

    with jax.named_scope("q_wait"):
        q_copy.wait()
        cnt_copy.wait()
    beta_copy(1).start()
    with jax.named_scope("diag"):
        cnt = cnt_v[...].astype(F32)
        row = lax.broadcasted_iota(jnp.int32, (natom, natom), 0)
        col = lax.broadcasted_iota(jnp.int32, (natom, natom), 1)
        offs = jnp.sum(jnp.where(col < row, cnt, 0.0), axis=1, keepdims=True)
        own = jnp.sum(jnp.where(col == row, cnt, 0.0), axis=1, keepdims=True)
        q_parts[...] = jnp.zeros_like(q_parts)
        for i in range(maxp):
            q = q_v[i]
            q_hi = q.astype(BF16)
            at = slice(i * mp, i * mp + maxp)
            q_parts[0, at] = q_hi
            q_parts[1, at] = (q - q_hi.astype(F32)).astype(BF16)

        def diagonals(c, _):
            lanes = 256
            nd = qd.shape[0]
            ids = (c * lanes + lax.broadcasted_iota(jnp.int32, (natom, lanes), 1)).astype(F32)
            owns = (offs <= ids) & (ids < offs + own)
            pos = jnp.sum(jnp.where(owns, ids - offs, 0.0), axis=0, keepdims=True)
            count = jnp.sum(
                jnp.where(owns, jnp.broadcast_to(own, owns.shape), 0.0), axis=0, keepdims=True
            )
            pick = jnp.where(owns, 1.0, 0.0).astype(BF16)
            flat = jnp.dot(q_parts[0], pick, preferred_element_type=F32)
            flat += jnp.dot(q_parts[1], pick, preferred_element_type=F32)
            q_row = jnp.zeros((mp, lanes), F32)
            for i in range(maxp):
                q_row = jnp.where(pos == float(i), flat[i * mp : (i + 1) * mp], q_row)
            at = pos + lax.broadcasted_iota(jnp.int32, (nd, lanes), 0).astype(F32) - float(maxp - 1)
            entries = jnp.zeros((nd, lanes), F32)
            for j in range(maxp):
                entries = jnp.where(at == float(j), q_row[j : j + 1], entries)
            qd[:, aligned(c, lanes)] = jnp.where(at < count, entries, 0.0)
            return 0

        for c in range(p_size // 256):
            diagonals(c, 0)
            if c == 2:
                beta_copy(2).start()

    with jax.named_scope("trial_wait"):
        trial_copy.wait()
    psi_copy(0).start()

    mine_t = pl.ds(pl.multiple_of(bw + band * cols, cols), cols)

    def turn(k, _):
        own = trial_v[aligned(k, sw), :].T
        trial_t[:, aligned(k, sw)] = own
        lhs[mine_t, aligned(k, sw)] = own
        return 0

    with jax.named_scope("turn"):
        for k in range(g // sw):
            turn(k, 0)

    trial_x = pltpu.make_async_remote_copy(
        src_ref=trial_t,
        dst_ref=lhs.at[mine_t, :],
        send_sem=xs,
        recv_sem=xr,
        **partner,
    )

    def flip(to, first, k, rows):
        part = pl.ds(pl.multiple_of(first + k * rows, rows), rows)
        to[aligned(k, rows), :] = beta_v[:, part].T

    def project(c, _):
        with jax.named_scope("load"):
            beta_copy(c).wait()
        at = aligned(c, bw)
        with jax.named_scope("p1"):
            part = jnp.dot(trial_t[...], beta_v[:, at], preferred_element_type=F32)
            flip(lhs, 0, jnp.minimum(c, 1), bw // 2)
            code, scale = encode(part)
            proj[:, :, :, :, :, at] = part.reshape(2, 2, 2, 2, r1, bw)
            code1[:, :, :, :, :, at] = code.reshape(2, 2, 2, 2, r1, bw)
            scale1[c] = scale

        @pl.when(c == 0)
        def _():
            with jax.named_scope("barrier"):
                pl.semaphore_wait(barrier, len(met) + 1)
            trial_x.start()

        for i in range(beta_chunks):
            near = routes[i % 3][0]
            now = pl.ds(i * bw, bw)

            @pl.when(c == i)
            def _():
                for d in peers:
                    send(
                        code1.at[pick(near, d) + (slice(None), now)], scale1.at[i],
                        in1.at[d, :, :, :, now], in1s.at[i, d], recv1.at[i], device(near, d),
                    )
                for k in ((1,), (2, 3), ())[i]:
                    psi_copy(k).start()

        return 0

    lax.fori_loop(0, beta_chunks, project, 0)

    def keep(got, first, k):
        top, rest = split2(got)
        at = (aligned(first, bw), aligned(k, pw))
        g_hi[at] = top
        g_lo[at] = rest

    with jax.named_scope("trial_x"):
        trial_x.wait()

    def early(k, _):
        @pl.when(k == 2)
        def _():
            for c in range(beta_chunks):
                with jax.named_scope(f"mid1_{c}"):
                    middle1(c)

        with jax.named_scope("psi_wait"):
            psi_copy(k).wait()
        with jax.named_scope("bands_0"):
            at = aligned(k, pw)
            flip(beta_t, bw, k, 2 * bw // psi_chunks)
            got = jnp.dot(lhs[...], psi_v[:, at], preferred_element_type=F32)
            keep(got[:bw], 0, k)
            fin[..., at] = got[bw:].reshape(2, 2, 2, 2, r2, pw)
        return 0

    lax.fori_loop(0, psi_chunks, early, 0)

    plane, line = routes[0]

    def share_w(at, recv, to):
        a, b = wall.at[at], walls.at[at]
        send(a, b, a, b, recv, to)

    def block(d):
        return (band,) + cell(line, d) + cell(plane, 0)

    def weigh():
        with jax.named_scope("wait_z1"):
            for c in range(beta_chunks):
                landed(late1, recv1b.at[c])

        with jax.named_scope("q_apply"):
            pieces = []
            for c in range(beta_chunks):
                at = pl.ds(c * bw, bw)
                piece = mid1[cell(routes[c % 3][1], 0) + (slice(None), at)]
                for d in peers:
                    piece += decode(end1[d, :, at], end1s[c, d])
                pieces.append(piece)
            x = jnp.concatenate(pieces, axis=1)
            acc = jnp.zeros_like(x)
            for d in range(2 * maxp - 1):
                shift = (maxp - 1 - d) % p_size
                moved = x if shift == 0 else pltpu.roll(x, shift, axis=1)
                acc += qd[d : d + 1, :] * moved
            tiles = [acc[:, t : t + 128] for t in range(0, p_size, 128)]
            top = functools.reduce(jnp.maximum, [jnp.abs(t) for t in tiles])
            top = jnp.max(top, axis=0, keepdims=True)
            code, scale = encode(acc, jnp.concatenate([top] * len(tiles), axis=1))
            wall[(band,) + pick((3, 2), 0)[:2] + pick((1, 0), 0)[2:]] = code
            walls[(band,) + pick((3, 2), 0)[:2] + pick((1, 0), 0)[2:]] = scale[:, :128]
        for d in peers:
            share_w(block(0), recv2.at[d - 1], device(line, d))
        for d in peers:
            share_w(block(0), recv2b.at[0], device(plane, d))

    def relay(e):
        landed(one, recv2.at[e - 1])
        for d in peers:
            share_w(block(e), recv2b.at[e], device(plane, d))

    def across(e):
        landed(3 * one, recv2b.at[e])
        row = (band,) + cell(line, e)
        a, b = wall.at[row], walls.at[row]
        send(a, b, a, b, recv2c.at[e], partner)

    def spread(b, e):
        high, low = cell(line, e)
        scale = jnp.concatenate([walls[b, high, low]] * (p_size // 128), axis=-1)
        values = decode(wall[b, high, low], scale)
        top, rest = split2(values.reshape(4 * r1, p_size))
        at = aligned(b * 4 + high * 2 + low, 4 * r1)
        w_hi[at, :] = top
        w_lo[at, :] = rest

    def late(u, _):
        for when, steps in (
            (1, (weigh,)),
            (3, (functools.partial(relay, 1),)),
            (4, (functools.partial(relay, 2),)),
            (5, (functools.partial(relay, 3), functools.partial(across, 0))),
            (6, (functools.partial(across, 1),)),
            (7, (functools.partial(across, 2),)),
        ):

            @pl.when(u == when)
            def _():
                with jax.named_scope(f"service_{when}"):
                    for step in steps:
                        step()

        with jax.named_scope("bands_1"):
            c, k = lax.div(u, psi_chunks), lax.rem(u, psi_chunks)
            rows = beta_t[aligned(c, bw), :]
            keep(jnp.dot(rows, psi_v[:, aligned(k, pw)], preferred_element_type=F32), c + 1, k)
        return 0

    lax.fori_loop(0, (beta_chunks - 1) * psi_chunks, late, 0)

    with jax.named_scope("ag_xy"):
        across(3)
    with jax.named_scope("spread_own"):
        for e in range(4):
            spread(band, e)
    with jax.named_scope("across"):
        for e in range(4):
            landed(4 * one, recv2c.at[e])
            spread(1 - band, e)

    def middle3(c):
        near, late = routes[c % 3]
        at = aligned(c, pw)
        landed(near3, recv3.at[c])
        total = fin[pick(near, 0) + (slice(None), at)].reshape(4 * r2, pw)
        for d in peers:
            total += decode(in3[d, :, :, :, at].reshape(4 * r2, pw), in3s[c, d])
        code, scale = encode(total)
        scale3b[c] = scale
        code3b[:, :, :, at] = code.reshape(2, 2, r2, pw)
        mid3[:, :, :, at] = total.reshape(2, 2, r2, pw)
        for d in peers:
            send(
                code3b.at[cell(late, d) + (slice(None), at)], scale3b.at[c],
                end3.at[d, :, at], end3s.at[c, d], recv3b.at[c], device(late, d),
            )

    def product(c):
        at = aligned(c, pw)
        f = jnp.dot(w_hi[...], g_hi[:, at], preferred_element_type=F32)
        f += jnp.dot(w_hi[...], g_lo[:, at], preferred_element_type=F32)
        f += jnp.dot(w_lo[...], g_hi[:, at], preferred_element_type=F32)
        return f + fin[..., at].reshape(2 * cols, pw)

    def share(c, _):
        at = aligned(c, pw)
        with jax.named_scope("share"):
            f = product(c)
            code, scale = encode(f)
            scale3[c] = scale
            code3[..., at] = code.reshape(2, 2, 2, 2, r2, pw)
            fin[..., at] = f.reshape(2, 2, 2, 2, r2, pw)
        for i in range(psi_chunks):
            near = routes[i % 3][0]
            now = pl.ds(i * pw, pw)

            @pl.when(c == i)
            def _():
                for d in peers:
                    send(
                        code3.at[pick(near, d) + (slice(None), now)], scale3.at[i],
                        in3.at[d, :, :, :, now], in3s.at[i, d], recv3.at[i], device(near, d),
                    )

        return 0

    lax.fori_loop(0, psi_chunks, share, 0)
    for c in range(psi_chunks):
        with jax.named_scope(f"mid3_{c}"):
            middle3(c)

    with jax.named_scope("tail"):
        for c in range(psi_chunks):
            at = aligned(c, pw)
            landed(late3, recv3b.at[c])
            total = mid3[cell(routes[c % 3][1], 0) + (slice(None), at)]
            for d in peers:
                total += decode(end3[d, :, at], end3s[c, d])
            out_ref[:, at] = total

    with jax.named_scope("drain"):
        total = beta_chunks * (near1 + late1) + psi_chunks * (near3 + late3) + 31 * one
        counted(total, recv1.at[0]).wait_send()


def fused(n, blk, psi, trial, beta, q_blocks, atom_counts):
    g, cols = trial.shape
    nbands = psi.shape[1]
    p_size = beta.shape[1]
    natom, maxp = q_blocks.shape[:2]
    mp = -(-maxp // 8) * 8
    nd = -(-(2 * maxp - 1) // 8) * 8
    r1, r2 = cols // n, blk // n
    bc, pc = 3, 4
    meter = (2 * (15 * (cols * p_size + blk * nbands) // 16) + 2 * 16 * cols * p_size) // 512 + 1024
    dma = pltpu.SemaphoreType.DMA
    vm = pltpu.VMEM
    out = pl.pallas_call(
        functools.partial(kernel, n, maxp),
        out_shape=jax.ShapeDtypeStruct((r2, nbands), F32),
        in_specs=[pl.BlockSpec(memory_space=pl.ANY)] * 5,
        out_specs=pl.BlockSpec(memory_space=pltpu.VMEM),
        scratch_shapes=[
            vm((g, nbands), BF16),
            vm((g, p_size), BF16),
            vm((g, cols), BF16),
            vm((maxp, maxp, natom), F32),
            vm((1, natom), jnp.int32),
            vm((p_size // bc + blk, g), BF16),
            vm((p_size - p_size // bc, g), BF16),
            vm((cols, g), BF16),
            vm((2, maxp * mp, natom), BF16),
            vm((nd, p_size), F32),
            vm((p_size, nbands), BF16),
            vm((p_size, nbands), BF16),
            vm((blk, p_size), BF16),
            vm((blk, p_size), BF16),
            vm((2, 2, 2, 2, r1, p_size), F32),
            vm((2, 2, 2, 2, r1, p_size), I16),
            vm((bc, 1, p_size // bc), F32),
            vm((4, 2, 2, r1, p_size), I16),
            vm((bc, 4, 1, p_size // bc), F32),
            vm((2, 2, r1, p_size), F32),
            vm((2, 2, r1, p_size), I16),
            vm((bc, 1, p_size // bc), F32),
            vm((4, r1, p_size), I16),
            vm((bc, 4, 1, p_size // bc), F32),
            vm((2, 2, 2, 2, 2, r1, p_size), I16),
            vm((2, 2, 2, 2, 2, 1, 128), F32),
            vm((2, 2, 2, 2, r2, nbands), F32),
            vm((2, 2, 2, 2, r2, nbands), I16),
            vm((pc, 1, nbands // pc), F32),
            vm((4, 2, 2, r2, nbands), I16),
            vm((pc, 4, 1, nbands // pc), F32),
            vm((2, 2, r2, nbands), F32),
            vm((2, 2, r2, nbands), I16),
            vm((pc, 1, nbands // pc), F32),
            vm((4, r2, nbands), I16),
            vm((pc, 4, 1, nbands // pc), F32),
            vm((meter, 1, 128), F32),
            dma((2,)),
            dma,
            dma((bc,)),
            dma((pc,)),
            dma,
            dma,
            dma,
            dma((bc,)),
            dma((bc,)),
            dma((3,)),
            dma((4,)),
            dma((4,)),
            dma((pc,)),
            dma((pc,)),
        ],
        compiler_params=pltpu.CompilerParams(
            collective_id=0, has_side_effects=True, vmem_limit_bytes=62 * 1024 * 1024
        ),
    )(psi, trial, beta, q_blocks.transpose(1, 2, 0), atom_counts.reshape(1, natom))
    return out.T


def q_dense(atom_counts, q_blocks, p_size):
    offsets = jnp.cumsum(atom_counts, dtype=jnp.int32) - atom_counts
    natom, maxp = q_blocks.shape[:2]
    ids = jnp.arange(p_size, dtype=jnp.int32)
    owns = (offsets[None, :] <= ids[:, None]) & (ids[:, None] < (offsets + atom_counts)[None, :])
    pos = jnp.sum(jnp.where(owns, ids[:, None] - offsets[None, :], 0), axis=1)
    atom = jnp.sum(jnp.where(owns, jnp.arange(natom, dtype=jnp.int32)[None, :], 0), axis=1)
    flat = jnp.dot(owns.astype(F32), q_blocks.reshape(natom, maxp * maxp), precision=precise)
    place = pos[:, None] == jnp.arange(maxp, dtype=jnp.int32)[None, :]
    rows = jnp.sum(jnp.where(place[:, :, None], flat.reshape(p_size, maxp, maxp), 0.0), axis=1)
    entries = jnp.dot(rows, place.astype(F32).T, precision=precise)
    return jnp.where(atom[:, None] == atom[None, :], entries, 0.0)


def general(psi, trial, beta, q_blocks, atom_counts):
    own = lax.psum(contract(beta, trial), "ga")
    weighted = jnp.dot(q_dense(atom_counts, q_blocks, beta.shape[1]), own, precision=precise)
    w_hi, w_lo = split2(weighted)
    both = jnp.dot(beta, jnp.concatenate([w_hi, w_lo], axis=1), preferred_element_type=F32)
    cols = trial.shape[1]
    s = both[:, :cols] + both[:, cols:] + trial.astype(F32)
    s_hi, s_lo = split2(lax.all_gather(s, "band", axis=1, tiled=True))
    part = contract(psi, s_hi) + contract(psi, s_lo)
    return lax.psum_scatter(part, "ga", scatter_dimension=1, tiled=True)


def solution(mesh):
    n, bands = mesh.shape["ga"], mesh.shape["band"]

    def shards(psi, trial, beta, q_blocks, atom_counts):
        g, cols = trial.shape
        blk = cols * bands
        fits = (
            bands == 2
            and n == 16
            and cols % 128 == 0
            and cols % (8 * n) == 0
            and blk % (8 * n) == 0
            and g % 4096 == 0
            and beta.shape[1] % 768 == 0
            and psi.shape[1] % 512 == 0
            and q_blocks.shape[0] % 128 == 0
        )
        if fits:
            return fused(n, blk, psi, trial, beta, q_blocks, atom_counts)
        return general(psi, trial, beta, q_blocks, atom_counts)

    in_specs = (P("ga", "band"), P("ga", "band"), P("ga", None), P(), P())
    out_specs = P("band", "ga")
    return jax.shard_map(shards, mesh=mesh, in_specs=in_specs, out_specs=out_specs, check_vma=False)
```

```python
import functools

import jax
import jax.numpy as jnp
from jax import lax
from jax.experimental import pallas as pl
from jax.experimental.pallas import tpu as pltpu
from jax.sharding import PartitionSpec as P

MESH = pl.DeviceIdType.MESH
precise = lax.Precision.HIGHEST
F32, BF16, I16 = jnp.float32, jnp.bfloat16, jnp.int16
LEVELS, TINY = 32767.0, 1e-30


def contract(left, right, precision=None):
    return lax.dot_general(
        left, right, (((0,), (0,)), ((), ())), precision=precision, preferred_element_type=F32
    )


def split2(x):
    hi = x.astype(BF16)
    return hi, (x - hi.astype(F32)).astype(BF16)


def encode(x, top=None):
    if top is None:
        top = jnp.max(jnp.abs(x), axis=0, keepdims=True)
    top = jnp.maximum(top, TINY)
    return jnp.round(x * (LEVELS / top)).astype(jnp.int32).astype(I16), top * (1.0 / LEVELS)


def decode(code, scale):
    return code.astype(jnp.int32).astype(F32) * scale


def kernel(
    n, maxp, psi_h, trial_h, beta_h, q_h, cnt_h, out_ref,
    psi_v, beta_v, trial_v, q_v, cnt_v, lhs, beta_t, trial_t, q_parts, qd, g_hi, g_lo, w_hi, w_lo,
    proj, code1, scale1, in1, in1s, mid1, code1b, scale1b, end1, end1s,
    wall, walls, fin, code3, scale3, in3, in3s, mid3, code3b, scale3b, end3, end3s, meter,
    q_sem, trial_sem, beta_sem, psi_sem, xs, xr, sent, recv1, recv1b, recv2, recv2b, recv2c,
    recv3, recv3b,
):
    me = lax.axis_index("ga")
    band = lax.axis_index("band")
    bit = [lax.rem(lax.div(me, 1 << p), 2) for p in range(4)]
    routes = (((1, 0), (3, 2)), ((2, 1), (3, 0)), ((2, 0), (3, 1)))
    peers = (3, 2, 1)

    def toggled(pair, d):
        return {p: lax.rem(bit[p] + (d >> k & 1), 2) for k, p in enumerate(pair[::-1])}

    def device(pair, d):
        there = sum((v - bit[p]) * (1 << p) for p, v in toggled(pair, d).items())
        return dict(device_id=(me + there, band), device_id_type=MESH)

    def pick(pair, d):
        bits = toggled(pair, d)
        return tuple(bits.get(p, slice(None)) for p in (3, 2, 1, 0))

    def cell(pair, d):
        bits = toggled(pair, d)
        return tuple(bits[p] for p in pair)

    partner = dict(device_id=(me, 1 - band), device_id_type=MESH)

    g, cols = trial_v.shape
    p_size = beta_v.shape[1]
    nbands = psi_v.shape[1]
    natom = cnt_v.shape[1]
    mp = q_parts.shape[1] // maxp
    r1 = cols // n
    r2 = out_ref.shape[0]
    beta_chunks = beta_sem.shape[0]
    bw = p_size // beta_chunks
    psi_chunks = psi_sem.shape[0]
    pw = nbands // psi_chunks
    sw = 512

    def aligned(i, size):
        return pl.ds(i * size if isinstance(i, int) else pl.multiple_of(i * size, size), size)

    def beta_copy(c):
        at = (slice(None), pl.ds(c * bw, bw))
        return pltpu.make_async_copy(beta_h.at[at], beta_v.at[at], beta_sem.at[c])

    def psi_copy(c):
        at = (slice(None), pl.ds(c * pw, pw))
        return pltpu.make_async_copy(psi_h.at[at], psi_v.at[at], psi_sem.at[c])

    q_copy = pltpu.make_async_copy(q_h, q_v, q_sem.at[0])
    cnt_copy = pltpu.make_async_copy(cnt_h, cnt_v, q_sem.at[1])
    trial_copy = pltpu.make_async_copy(trial_h, trial_v, trial_sem)
    q_copy.start()
    cnt_copy.start()
    trial_copy.start()
    beta_copy(0).start()

    barrier = pltpu.get_barrier_semaphore()

    met = [(pair, d) for pair in routes[0] for d in peers]
    met += [(pair, 3) for route in routes[1:] for pair in route]
    for pair, d in met:
        pl.semaphore_signal(barrier, inc=1, **device(pair, d))
    pl.semaphore_signal(barrier, inc=1, **partner)

    def send(src, src_s, dst, dst_s, recv, to):
        for a, b in ((src, dst), (src_s, dst_s)):
            pltpu.make_async_remote_copy(
                src_ref=a, dst_ref=b, send_sem=sent, recv_sem=recv, **to
            ).start()

    def size(values, lanes, copies):
        return copies * (2 * values + 4 * lanes) // (4 * 128)

    def counted(rows, recv):
        a = meter.at[pl.ds(0, rows)]
        return pltpu.make_async_remote_copy(
            src_ref=a, dst_ref=a, send_sem=sent, recv_sem=recv, **partner
        )

    def landed(rows, recv):
        counted(rows, recv).wait_recv()

    near1, late1 = size(4 * r1 * bw, bw, 3), size(r1 * bw, bw, 3)
    near3, late3 = size(4 * r2 * pw, pw, 3), size(r2 * pw, pw, 3)
    one = size(r1 * p_size, 128, 1)

    def middle1(c):
        near, late = routes[c % 3]
        at = pl.ds(c * bw, bw)
        landed(near1, recv1.at[c])
        total = proj[pick(near, 0) + (slice(None), at)].reshape(4 * r1, bw)
        for d in peers:
            total += decode(in1[d, :, :, :, at].reshape(4 * r1, bw), in1s[c, d])
        code, scale = encode(total)
        scale1b[c] = scale
        code1b[:, :, :, at] = code.reshape(2, 2, r1, bw)
        mid1[:, :, :, at] = total.reshape(2, 2, r1, bw)
        for d in peers:
            send(
                code1b.at[cell(late, d) + (slice(None), at)], scale1b.at[c],
                end1.at[d, :, at], end1s.at[c, d], recv1b, device(late, d),
            )

    with jax.named_scope("q_wait"):
        q_copy.wait()
        cnt_copy.wait()
    beta_copy(1).start()
    with jax.named_scope("diag"):
        cnt = cnt_v[...].astype(F32)
        row = lax.broadcasted_iota(jnp.int32, (natom, natom), 0)
        col = lax.broadcasted_iota(jnp.int32, (natom, natom), 1)
        offs = jnp.sum(jnp.where(col < row, cnt, 0.0), axis=1, keepdims=True)
        own = jnp.sum(jnp.where(col == row, cnt, 0.0), axis=1, keepdims=True)
        q_parts[...] = jnp.zeros_like(q_parts)
        for i in range(maxp):
            q = q_v[i]
            q_hi = q.astype(BF16)
            at = slice(i * mp, i * mp + maxp)
            q_parts[0, at] = q_hi
            q_parts[1, at] = (q - q_hi.astype(F32)).astype(BF16)

        def diagonals(c, _):
            lanes = 256
            nd = qd.shape[0]
            ids = (c * lanes + lax.broadcasted_iota(jnp.int32, (natom, lanes), 1)).astype(F32)
            owns = (offs <= ids) & (ids < offs + own)
            pos = jnp.sum(jnp.where(owns, ids - offs, 0.0), axis=0, keepdims=True)
            count = jnp.sum(
                jnp.where(owns, jnp.broadcast_to(own, owns.shape), 0.0), axis=0, keepdims=True
            )
            pick = jnp.where(owns, 1.0, 0.0).astype(BF16)
            flat = jnp.dot(q_parts[0], pick, preferred_element_type=F32)
            flat += jnp.dot(q_parts[1], pick, preferred_element_type=F32)
            q_row = jnp.zeros((mp, lanes), F32)
            for i in range(maxp):
                q_row = jnp.where(pos == float(i), flat[i * mp : (i + 1) * mp], q_row)
            at = pos + lax.broadcasted_iota(jnp.int32, (nd, lanes), 0).astype(F32) - float(maxp - 1)
            entries = jnp.zeros((nd, lanes), F32)
            for j in range(maxp):
                entries = jnp.where(at == float(j), q_row[j : j + 1], entries)
            qd[:, aligned(c, lanes)] = jnp.where(at < count, entries, 0.0)
            return 0

        for c in range(p_size // 256):
            diagonals(c, 0)
            if c == 2:
                beta_copy(2).start()

    with jax.named_scope("trial_wait"):
        trial_copy.wait()
    psi_copy(0).start()

    mine_t = pl.ds(pl.multiple_of(bw + band * cols, cols), cols)

    def turn(k, _):
        own = trial_v[aligned(k, sw), :].T
        trial_t[:, aligned(k, sw)] = own
        lhs[mine_t, aligned(k, sw)] = own
        return 0

    with jax.named_scope("turn"):
        for k in range(g // sw):
            turn(k, 0)

    trial_x = pltpu.make_async_remote_copy(
        src_ref=trial_t,
        dst_ref=lhs.at[mine_t, :],
        send_sem=xs,
        recv_sem=xr,
        **partner,
    )

    def flip(to, first, k, rows):
        part = pl.ds(pl.multiple_of(first + k * rows, rows), rows)
        to[aligned(k, rows), :] = beta_v[:, part].T

    def project(c, _):
        with jax.named_scope("load"):
            beta_copy(c).wait()
        at = aligned(c, bw)
        with jax.named_scope("p1"):
            part = jnp.dot(trial_t[...], beta_v[:, at], preferred_element_type=F32)
            flip(lhs, 0, jnp.minimum(c, 1), bw // 2)
            code, scale = encode(part)
            proj[:, :, :, :, :, at] = part.reshape(2, 2, 2, 2, r1, bw)
            code1[:, :, :, :, :, at] = code.reshape(2, 2, 2, 2, r1, bw)
            scale1[c] = scale

        @pl.when(c == 0)
        def _():
            with jax.named_scope("barrier"):
                pl.semaphore_wait(barrier, len(met) + 1)
            trial_x.start()

        for i in range(beta_chunks):
            near = routes[i % 3][0]
            now = pl.ds(i * bw, bw)

            @pl.when(c == i)
            def _():
                for d in peers:
                    send(
                        code1.at[pick(near, d) + (slice(None), now)], scale1.at[i],
                        in1.at[d, :, :, :, now], in1s.at[i, d], recv1.at[i], device(near, d),
                    )
                for k in ((1,), (2, 3), ())[i]:
                    psi_copy(k).start()

        return 0

    lax.fori_loop(0, beta_chunks, project, 0)

    def keep(got, first, k):
        top, rest = split2(got)
        at = (aligned(first, bw), aligned(k, pw))
        g_hi[at] = top
        g_lo[at] = rest

    with jax.named_scope("trial_x"):
        trial_x.wait()

    def early(k, _):
        @pl.when(k == 2)
        def _():
            for c in range(beta_chunks):
                with jax.named_scope(f"mid1_{c}"):
                    middle1(c)

        with jax.named_scope("psi_wait"):
            psi_copy(k).wait()
        with jax.named_scope("bands_0"):
            at = aligned(k, pw)
            flip(beta_t, bw, k, 2 * bw // psi_chunks)
            got = jnp.dot(lhs[...], psi_v[:, at], preferred_element_type=F32)
            keep(got[:bw], 0, k)
            fin[..., at] = got[bw:].reshape(2, 2, 2, 2, r2, pw)
        return 0

    lax.fori_loop(0, psi_chunks, early, 0)

    tracks = [(c, pl.ds(c * bw, bw)) + routes[c % 3] for c in range(beta_chunks)]

    def block(plane, line, e):
        bits = {**toggled(plane, 0), **toggled(line, e)}
        return (band,) + tuple(bits[p] for p in (3, 2, 1, 0))

    def share_w(c, at, lanes, recv, to):
        pieces = [wall.at[at + (slice(None), lanes)]]
        if c == 0:
            pieces.append(walls.at[at])
        for a in pieces:
            pltpu.make_async_remote_copy(
                src_ref=a, dst_ref=a, send_sem=sent, recv_sem=recv, **to
            ).start()

    def weigh():
        with jax.named_scope("wait_z1"):
            landed(beta_chunks * late1, recv1b)

        with jax.named_scope("q_apply"):
            pieces = []
            for c in range(beta_chunks):
                at = pl.ds(c * bw, bw)
                piece = mid1[cell(routes[c % 3][1], 0) + (slice(None), at)]
                for d in peers:
                    piece += decode(end1[d, :, at], end1s[c, d])
                pieces.append(piece)
            x = jnp.concatenate(pieces, axis=1)
            acc = jnp.zeros_like(x)
            for d in range(2 * maxp - 1):
                shift = (maxp - 1 - d) % p_size
                moved = x if shift == 0 else pltpu.roll(x, shift, axis=1)
                acc += qd[d : d + 1, :] * moved
            tiles = [acc[:, t : t + 128] for t in range(0, p_size, 128)]
            top = functools.reduce(jnp.maximum, [jnp.abs(t) for t in tiles])
            top = jnp.max(top, axis=0, keepdims=True)
            code, scale = encode(acc, jnp.concatenate([top] * len(tiles), axis=1))
            home = block((1, 0), (3, 2), 0)
            wall[home] = code
            walls[home] = scale[:, :128]
        for d in peers:
            for c, lanes, plane, line in tracks:
                share_w(c, block(plane, line, 0), lanes, recv2.at[d - 1], device(line, d))
        for d in peers:
            for c, lanes, plane, line in tracks:
                share_w(c, block(plane, line, 0), lanes, recv2b.at[0], device(plane, d))

    def relay(e):
        landed(one, recv2.at[e - 1])
        for d in peers:
            for c, lanes, plane, line in tracks:
                share_w(c, block(plane, line, e), lanes, recv2b.at[e], device(plane, d))

    def across(e):
        landed(3 * one, recv2b.at[e])
        for c, lanes, plane, line in tracks:
            share_w(c, (band,) + pick(line, e), lanes, recv2c, partner)

    def spread(b, high, low):
        scale = jnp.concatenate([walls[b, high, low]] * (p_size // 128), axis=-1)
        values = decode(wall[b, high, low], scale)
        top, rest = split2(values.reshape(4 * r1, p_size))
        at = aligned(b * 4 + high * 2 + low, 4 * r1)
        w_hi[at, :] = top
        w_lo[at, :] = rest

    def late(u, _):
        for when, steps in (
            (1, (weigh,)),
            (4, tuple(functools.partial(relay, e) for e in (1, 2, 3))),
            (5, (functools.partial(across, 0),)),
            (7, (functools.partial(across, 1),)),
        ):

            @pl.when(u == when)
            def _():
                with jax.named_scope(f"service_{when}"):
                    for step in steps:
                        step()

        with jax.named_scope("bands_1"):
            c, k = lax.div(u, psi_chunks), lax.rem(u, psi_chunks)
            rows = beta_t[aligned(c, bw), :]
            keep(jnp.dot(rows, psi_v[:, aligned(k, pw)], preferred_element_type=F32), c + 1, k)
        return 0

    lax.fori_loop(0, (beta_chunks - 1) * psi_chunks, late, 0)

    with jax.named_scope("ag_xy"):
        across(2)
        across(3)
    with jax.named_scope("spread_own"):
        for i in range(4):
            spread(band, i // 2, i % 2)
    with jax.named_scope("across"):
        landed(16 * one, recv2c)
        for i in range(4):
            spread(1 - band, i // 2, i % 2)

    def middle3(c):
        near, late = routes[c % 3]
        at = aligned(c, pw)
        landed(near3, recv3.at[c])
        total = fin[pick(near, 0) + (slice(None), at)].reshape(4 * r2, pw)
        for d in peers:
            total += decode(in3[d, :, :, :, at].reshape(4 * r2, pw), in3s[c, d])
        code, scale = encode(total)
        scale3b[c] = scale
        code3b[:, :, :, at] = code.reshape(2, 2, r2, pw)
        mid3[:, :, :, at] = total.reshape(2, 2, r2, pw)
        for d in peers:
            send(
                code3b.at[cell(late, d) + (slice(None), at)], scale3b.at[c],
                end3.at[d, :, at], end3s.at[c, d], recv3b.at[c], device(late, d),
            )

    def product(c):
        at = aligned(c, pw)
        f = jnp.dot(w_hi[...], g_hi[:, at], preferred_element_type=F32)
        f += jnp.dot(w_hi[...], g_lo[:, at], preferred_element_type=F32)
        f += jnp.dot(w_lo[...], g_hi[:, at], preferred_element_type=F32)
        return f + fin[..., at].reshape(2 * cols, pw)

    def share(c, _):
        at = aligned(c, pw)
        with jax.named_scope("share"):
            f = product(c)
            code, scale = encode(f)
            scale3[c] = scale
            code3[..., at] = code.reshape(2, 2, 2, 2, r2, pw)
            fin[..., at] = f.reshape(2, 2, 2, 2, r2, pw)
        for i in range(psi_chunks):
            near = routes[i % 3][0]
            now = pl.ds(i * pw, pw)

            @pl.when(c == i)
            def _():
                for d in peers:
                    send(
                        code3.at[pick(near, d) + (slice(None), now)], scale3.at[i],
                        in3.at[d, :, :, :, now], in3s.at[i, d], recv3.at[i], device(near, d),
                    )

        return 0

    lax.fori_loop(0, psi_chunks, share, 0)
    for c in range(psi_chunks):
        with jax.named_scope(f"mid3_{c}"):
            middle3(c)

    with jax.named_scope("tail"):
        for c in range(psi_chunks):
            at = aligned(c, pw)
            landed(late3, recv3b.at[c])
            total = mid3[cell(routes[c % 3][1], 0) + (slice(None), at)]
            for d in peers:
                total += decode(end3[d, :, at], end3s[c, d])
            out_ref[:, at] = total

    with jax.named_scope("drain"):
        total = beta_chunks * (near1 + late1) + psi_chunks * (near3 + late3) + 31 * one
        counted(total, recv1.at[0]).wait_send()


def fused(n, blk, psi, trial, beta, q_blocks, atom_counts):
    g, cols = trial.shape
    nbands = psi.shape[1]
    p_size = beta.shape[1]
    natom, maxp = q_blocks.shape[:2]
    mp = -(-maxp // 8) * 8
    nd = -(-(2 * maxp - 1) // 8) * 8
    r1, r2 = cols // n, blk // n
    bc, pc = 3, 4
    meter = (2 * (15 * (cols * p_size + blk * nbands) // 16) + 2 * 16 * cols * p_size) // 512 + 1024
    dma = pltpu.SemaphoreType.DMA
    vm = pltpu.VMEM
    out = pl.pallas_call(
        functools.partial(kernel, n, maxp),
        out_shape=jax.ShapeDtypeStruct((r2, nbands), F32),
        in_specs=[pl.BlockSpec(memory_space=pl.ANY)] * 5,
        out_specs=pl.BlockSpec(memory_space=pltpu.VMEM),
        scratch_shapes=[
            vm((g, nbands), BF16),
            vm((g, p_size), BF16),
            vm((g, cols), BF16),
            vm((maxp, maxp, natom), F32),
            vm((1, natom), jnp.int32),
            vm((p_size // bc + blk, g), BF16),
            vm((p_size - p_size // bc, g), BF16),
            vm((cols, g), BF16),
            vm((2, maxp * mp, natom), BF16),
            vm((nd, p_size), F32),
            vm((p_size, nbands), BF16),
            vm((p_size, nbands), BF16),
            vm((blk, p_size), BF16),
            vm((blk, p_size), BF16),
            vm((2, 2, 2, 2, r1, p_size), F32),
            vm((2, 2, 2, 2, r1, p_size), I16),
            vm((bc, 1, p_size // bc), F32),
            vm((4, 2, 2, r1, p_size), I16),
            vm((bc, 4, 1, p_size // bc), F32),
            vm((2, 2, r1, p_size), F32),
            vm((2, 2, r1, p_size), I16),
            vm((bc, 1, p_size // bc), F32),
            vm((4, r1, p_size), I16),
            vm((bc, 4, 1, p_size // bc), F32),
            vm((2, 2, 2, 2, 2, r1, p_size), I16),
            vm((2, 2, 2, 2, 2, 1, 128), F32),
            vm((2, 2, 2, 2, r2, nbands), F32),
            vm((2, 2, 2, 2, r2, nbands), I16),
            vm((pc, 1, nbands // pc), F32),
            vm((4, 2, 2, r2, nbands), I16),
            vm((pc, 4, 1, nbands // pc), F32),
            vm((2, 2, r2, nbands), F32),
            vm((2, 2, r2, nbands), I16),
            vm((pc, 1, nbands // pc), F32),
            vm((4, r2, nbands), I16),
            vm((pc, 4, 1, nbands // pc), F32),
            vm((meter, 1, 128), F32),
            dma((2,)),
            dma,
            dma((bc,)),
            dma((pc,)),
            dma,
            dma,
            dma,
            dma((bc,)),
            dma,
            dma((3,)),
            dma((4,)),
            dma,
            dma((pc,)),
            dma((pc,)),
        ],
        compiler_params=pltpu.CompilerParams(
            collective_id=0, has_side_effects=True, vmem_limit_bytes=62 * 1024 * 1024
        ),
    )(psi, trial, beta, q_blocks.transpose(1, 2, 0), atom_counts.reshape(1, natom))
    return out.T


def q_dense(atom_counts, q_blocks, p_size):
    offsets = jnp.cumsum(atom_counts, dtype=jnp.int32) - atom_counts
    natom, maxp = q_blocks.shape[:2]
    ids = jnp.arange(p_size, dtype=jnp.int32)
    owns = (offsets[None, :] <= ids[:, None]) & (ids[:, None] < (offsets + atom_counts)[None, :])
    pos = jnp.sum(jnp.where(owns, ids[:, None] - offsets[None, :], 0), axis=1)
    atom = jnp.sum(jnp.where(owns, jnp.arange(natom, dtype=jnp.int32)[None, :], 0), axis=1)
    flat = jnp.dot(owns.astype(F32), q_blocks.reshape(natom, maxp * maxp), precision=precise)
    place = pos[:, None] == jnp.arange(maxp, dtype=jnp.int32)[None, :]
    rows = jnp.sum(jnp.where(place[:, :, None], flat.reshape(p_size, maxp, maxp), 0.0), axis=1)
    entries = jnp.dot(rows, place.astype(F32).T, precision=precise)
    return jnp.where(atom[:, None] == atom[None, :], entries, 0.0)


def general(psi, trial, beta, q_blocks, atom_counts):
    own = lax.psum(contract(beta, trial), "ga")
    weighted = jnp.dot(q_dense(atom_counts, q_blocks, beta.shape[1]), own, precision=precise)
    w_hi, w_lo = split2(weighted)
    both = jnp.dot(beta, jnp.concatenate([w_hi, w_lo], axis=1), preferred_element_type=F32)
    cols = trial.shape[1]
    s = both[:, :cols] + both[:, cols:] + trial.astype(F32)
    s_hi, s_lo = split2(lax.all_gather(s, "band", axis=1, tiled=True))
    part = contract(psi, s_hi) + contract(psi, s_lo)
    return lax.psum_scatter(part, "ga", scatter_dimension=1, tiled=True)


def solution(mesh):
    n, bands = mesh.shape["ga"], mesh.shape["band"]

    def shards(psi, trial, beta, q_blocks, atom_counts):
        g, cols = trial.shape
        blk = cols * bands
        fits = (
            bands == 2
            and n == 16
            and cols % 128 == 0
            and cols % (8 * n) == 0
            and blk % (8 * n) == 0
            and g % 4096 == 0
            and beta.shape[1] % 768 == 0
            and psi.shape[1] % 512 == 0
            and q_blocks.shape[0] % 128 == 0
        )
        if fits:
            return fused(n, blk, psi, trial, beta, q_blocks, atom_counts)
        return general(psi, trial, beta, q_blocks, atom_counts)

    in_specs = (P("ga", "band"), P("ga", "band"), P("ga", None), P(), P())
    out_specs = P("band", "ga")
    return jax.shard_map(shards, mesh=mesh, in_specs=in_specs, out_specs=out_specs, check_vma=False)
```

```python
import functools

import jax
import jax.numpy as jnp
from jax import lax
from jax.experimental import pallas as pl
from jax.experimental.pallas import tpu as pltpu
from jax.sharding import PartitionSpec as P

MESH = pl.DeviceIdType.MESH
precise = lax.Precision.HIGHEST
F32, BF16, I16 = jnp.float32, jnp.bfloat16, jnp.int16
LEVELS, TINY = 32767.0, 4e-34


def contract(left, right, precision=None):
    return lax.dot_general(
        left, right, (((0,), (0,)), ((), ())), precision=precision, preferred_element_type=F32
    )


def split2(x):
    hi = x.astype(BF16)
    return hi, (x - hi.astype(F32)).astype(BF16)


def encode(x, top=None):
    if top is None:
        top = jnp.max(jnp.abs(x), axis=0, keepdims=True)
    top = jnp.maximum(top, TINY)
    return jnp.round(x * (LEVELS / top)).astype(jnp.int32).astype(I16), top * (1.0 / LEVELS)


def decode(code, scale):
    return code.astype(jnp.int32).astype(F32) * scale


def kernel(
    n, maxp, psi_h, trial_h, beta_h, q_h, cnt_h, out_ref,
    psi_v, beta_v, trial_v, q_v, cnt_v, lhs, beta_t, trial_t, q_parts, qd, g_hi, g_lo, w_hi, w_lo,
    proj, code1, scale1, in1, in1s, mid1, code1b, scale1b, end1, end1s,
    wall, walls, fin, code3, scale3, in3, in3s, mid3, code3b, scale3b, end3, end3s, meter,
    q_sem, trial_sem, beta_sem, psi_sem, xs, xr, sent, recv1, recv1b, recv2, recv2b, recv2c,
    recv3, recv3b,
):
    me = lax.axis_index("ga")
    band = lax.axis_index("band")
    bit = [lax.rem(lax.div(me, 1 << p), 2) for p in range(4)]
    routes = (((1, 0), (3, 2)), ((2, 1), (3, 0)), ((2, 0), (3, 1)))
    peers = (3, 2, 1)

    def toggled(pair, d):
        return {p: lax.rem(bit[p] + (d >> k & 1), 2) for k, p in enumerate(pair[::-1])}

    def device(pair, d):
        there = sum((v - bit[p]) * (1 << p) for p, v in toggled(pair, d).items())
        return dict(device_id=(me + there, band), device_id_type=MESH)

    def pick(pair, d):
        bits = toggled(pair, d)
        return tuple(bits.get(p, slice(None)) for p in (3, 2, 1, 0))

    def cell(pair, d):
        bits = toggled(pair, d)
        return tuple(bits[p] for p in pair)

    partner = dict(device_id=(me, 1 - band), device_id_type=MESH)

    g, cols = trial_v.shape
    p_size = beta_v.shape[1]
    nbands = psi_v.shape[1]
    natom = cnt_v.shape[1]
    mp = q_parts.shape[1] // maxp
    r1 = cols // n
    r2 = out_ref.shape[0]
    beta_chunks = beta_sem.shape[0]
    bw = p_size // beta_chunks
    psi_chunks = psi_sem.shape[0]
    pw = nbands // psi_chunks
    sw = 512

    def aligned(i, size):
        return pl.ds(i * size if isinstance(i, int) else pl.multiple_of(i * size, size), size)

    def beta_copy(c):
        at = (slice(None), pl.ds(c * bw, bw))
        return pltpu.make_async_copy(beta_h.at[at], beta_v.at[at], beta_sem.at[c])

    def psi_copy(c):
        at = (slice(None), pl.ds(c * pw, pw))
        return pltpu.make_async_copy(psi_h.at[at], psi_v.at[at], psi_sem.at[c])

    q_copy = pltpu.make_async_copy(q_h, q_v, q_sem.at[0])
    cnt_copy = pltpu.make_async_copy(cnt_h, cnt_v, q_sem.at[1])
    trial_copy = pltpu.make_async_copy(trial_h, trial_v, trial_sem)
    q_copy.start()
    cnt_copy.start()
    trial_copy.start()
    beta_copy(0).start()

    barrier = pltpu.get_barrier_semaphore()

    met = [(pair, d) for pair in routes[0] for d in peers]
    met += [(pair, 3) for route in routes[1:] for pair in route]
    for pair, d in met:
        pl.semaphore_signal(barrier, inc=1, **device(pair, d))
    pl.semaphore_signal(barrier, inc=1, **partner)

    def send(src, src_s, dst, dst_s, recv, to):
        for a, b in ((src, dst), (src_s, dst_s)):
            pltpu.make_async_remote_copy(
                src_ref=a, dst_ref=b, send_sem=sent, recv_sem=recv, **to
            ).start()

    def size(values, lanes, copies):
        return copies * (2 * values + 4 * lanes) // (4 * 128)

    def counted(rows, recv):
        a = meter.at[pl.ds(0, rows)]
        return pltpu.make_async_remote_copy(
            src_ref=a, dst_ref=a, send_sem=sent, recv_sem=recv, **partner
        )

    def landed(rows, recv):
        counted(rows, recv).wait_recv()

    near1, late1 = size(4 * r1 * bw, bw, 3), size(r1 * bw, bw, 3)
    near3, late3 = size(4 * r2 * pw, pw, 3), size(r2 * pw, pw, 3)
    one = size(r1 * p_size, 128, 1)

    def middle1(c):
        near, late = routes[c % 3]
        at = pl.ds(c * bw, bw)
        landed(near1, recv1.at[c])
        total = proj[pick(near, 0) + (slice(None), at)].reshape(4 * r1, bw)
        for d in peers:
            total += decode(in1[d, :, :, :, at].reshape(4 * r1, bw), in1s[c, d])
        code, scale = encode(total)
        scale1b[c] = scale
        code1b[:, :, :, at] = code.reshape(2, 2, r1, bw)
        mid1[:, :, :, at] = total.reshape(2, 2, r1, bw)
        for d in peers:
            send(
                code1b.at[cell(late, d) + (slice(None), at)], scale1b.at[c],
                end1.at[d, :, at], end1s.at[c, d], recv1b, device(late, d),
            )

    with jax.named_scope("q_wait"):
        q_copy.wait()
        cnt_copy.wait()
    beta_copy(1).start()
    with jax.named_scope("diag"):
        cnt = cnt_v[...].astype(F32)
        row = lax.broadcasted_iota(jnp.int32, (natom, natom), 0)
        col = lax.broadcasted_iota(jnp.int32, (natom, natom), 1)
        offs = jnp.sum(jnp.where(col < row, cnt, 0.0), axis=1, keepdims=True)
        own = jnp.sum(jnp.where(col == row, cnt, 0.0), axis=1, keepdims=True)
        q_parts[...] = jnp.zeros_like(q_parts)
        for i in range(maxp):
            q = q_v[i]
            q_hi = q.astype(BF16)
            at = slice(i * mp, i * mp + maxp)
            q_parts[0, at] = q_hi
            q_parts[1, at] = (q - q_hi.astype(F32)).astype(BF16)

        def diagonals(c, _):
            lanes = 256
            nd = qd.shape[0]
            ids = (c * lanes + lax.broadcasted_iota(jnp.int32, (natom, lanes), 1)).astype(F32)
            owns = (offs <= ids) & (ids < offs + own)
            pos = jnp.sum(jnp.where(owns, ids - offs, 0.0), axis=0, keepdims=True)
            count = jnp.sum(
                jnp.where(owns, jnp.broadcast_to(own, owns.shape), 0.0), axis=0, keepdims=True
            )
            pick = jnp.where(owns, 1.0, 0.0).astype(BF16)
            flat = jnp.dot(q_parts[0], pick, preferred_element_type=F32)
            flat += jnp.dot(q_parts[1], pick, preferred_element_type=F32)
            q_row = jnp.zeros((mp, lanes), F32)
            for i in range(maxp):
                q_row = jnp.where(pos == float(i), flat[i * mp : (i + 1) * mp], q_row)
            at = pos + lax.broadcasted_iota(jnp.int32, (nd, lanes), 0).astype(F32) - float(maxp - 1)
            entries = jnp.zeros((nd, lanes), F32)
            for j in range(maxp):
                entries = jnp.where(at == float(j), q_row[j : j + 1], entries)
            qd[:, aligned(c, lanes)] = jnp.where(at < count, entries, 0.0)
            return 0

        for c in range(p_size // 256):
            diagonals(c, 0)
            if c == 2:
                beta_copy(2).start()

    with jax.named_scope("trial_wait"):
        trial_copy.wait()
    psi_copy(0).start()

    mine_t = pl.ds(pl.multiple_of(bw + band * cols, cols), cols)

    def turn(k, _):
        own = trial_v[aligned(k, sw), :].T
        trial_t[:, aligned(k, sw)] = own
        lhs[mine_t, aligned(k, sw)] = own
        return 0

    with jax.named_scope("turn"):
        for k in range(g // sw):
            turn(k, 0)

    trial_x = pltpu.make_async_remote_copy(
        src_ref=trial_t,
        dst_ref=lhs.at[mine_t, :],
        send_sem=xs,
        recv_sem=xr,
        **partner,
    )

    def flip(to, first, k, rows):
        part = pl.ds(pl.multiple_of(first + k * rows, rows), rows)
        to[aligned(k, rows), :] = beta_v[:, part].T

    def project(c, _):
        with jax.named_scope("load"):
            beta_copy(c).wait()
        at = aligned(c, bw)
        with jax.named_scope("p1"):
            part = jnp.dot(trial_t[...], beta_v[:, at], preferred_element_type=F32)
            flip(lhs, 0, jnp.minimum(c, 1), bw // 2)
            code, scale = encode(part)
            proj[:, :, :, :, :, at] = part.reshape(2, 2, 2, 2, r1, bw)
            code1[:, :, :, :, :, at] = code.reshape(2, 2, 2, 2, r1, bw)
            scale1[c] = scale

        @pl.when(c == 0)
        def _():
            with jax.named_scope("barrier"):
                pl.semaphore_wait(barrier, len(met) + 1)
            trial_x.start()

        for i in range(beta_chunks):
            near = routes[i % 3][0]
            now = pl.ds(i * bw, bw)

            @pl.when(c == i)
            def _():
                for d in peers:
                    send(
                        code1.at[pick(near, d) + (slice(None), now)], scale1.at[i],
                        in1.at[d, :, :, :, now], in1s.at[i, d], recv1.at[i], device(near, d),
                    )
                for k in ((1,), (2, 3), ())[i]:
                    psi_copy(k).start()

        return 0

    lax.fori_loop(0, beta_chunks, project, 0)

    def keep(got, first, k):
        top, rest = split2(got)
        at = (aligned(first, bw), aligned(k, pw))
        g_hi[at] = top
        g_lo[at] = rest

    with jax.named_scope("trial_x"):
        trial_x.wait()

    def early(k, _):
        @pl.when(k == 2)
        def _():
            for c in range(beta_chunks):
                with jax.named_scope(f"mid1_{c}"):
                    middle1(c)

        with jax.named_scope("psi_wait"):
            psi_copy(k).wait()
        with jax.named_scope("bands_0"):
            at = aligned(k, pw)
            flip(beta_t, bw, k, 2 * bw // psi_chunks)
            got = jnp.dot(lhs[...], psi_v[:, at], preferred_element_type=F32)
            keep(got[:bw], 0, k)
            fin[..., at] = got[bw:].reshape(2, 2, 2, 2, r2, pw)
        return 0

    lax.fori_loop(0, psi_chunks, early, 0)

    tracks = [(c, pl.ds(c * bw, bw)) + routes[c % 3] for c in range(beta_chunks)]

    def block(plane, line, e):
        bits = {**toggled(plane, 0), **toggled(line, e)}
        return (band,) + tuple(bits[p] for p in (3, 2, 1, 0))

    def share_w(c, at, lanes, recv, to):
        pieces = [wall.at[at + (slice(None), lanes)]]
        if c == 0:
            pieces.append(walls.at[at])
        for a in pieces:
            pltpu.make_async_remote_copy(
                src_ref=a, dst_ref=a, send_sem=sent, recv_sem=recv, **to
            ).start()

    def weigh():
        with jax.named_scope("wait_z1"):
            landed(beta_chunks * late1, recv1b)

        with jax.named_scope("q_apply"):
            pieces = []
            for c in range(beta_chunks):
                at = pl.ds(c * bw, bw)
                piece = mid1[cell(routes[c % 3][1], 0) + (slice(None), at)]
                for d in peers:
                    piece += decode(end1[d, :, at], end1s[c, d])
                pieces.append(piece)
            x = jnp.concatenate(pieces, axis=1)
            acc = jnp.zeros_like(x)
            for d in range(2 * maxp - 1):
                shift = (maxp - 1 - d) % p_size
                moved = x if shift == 0 else pltpu.roll(x, shift, axis=1)
                acc += qd[d : d + 1, :] * moved
            tiles = [acc[:, t : t + 128] for t in range(0, p_size, 128)]
            top = functools.reduce(jnp.maximum, [jnp.abs(t) for t in tiles])
            top = jnp.max(top, axis=0, keepdims=True)
            code, scale = encode(acc, jnp.concatenate([top] * len(tiles), axis=1))
            home = block((1, 0), (3, 2), 0)
            wall[home] = code
            walls[home] = scale[:, :128]
        for d in peers:
            for c, lanes, plane, line in tracks:
                share_w(c, block(plane, line, 0), lanes, recv2.at[d - 1], device(line, d))
        for d in peers:
            for c, lanes, plane, line in tracks:
                share_w(c, block(plane, line, 0), lanes, recv2b.at[0], device(plane, d))

    def relay(e):
        landed(one, recv2.at[e - 1])
        for d in peers:
            for c, lanes, plane, line in tracks:
                share_w(c, block(plane, line, e), lanes, recv2b.at[e], device(plane, d))

    def across(e):
        landed(3 * one, recv2b.at[e])
        for c, lanes, plane, line in tracks:
            share_w(c, (band,) + pick(line, e), lanes, recv2c, partner)

    def spread(b, high, low):
        scale = jnp.concatenate([walls[b, high, low]] * (p_size // 128), axis=-1)
        values = decode(wall[b, high, low], scale)
        top, rest = split2(values.reshape(4 * r1, p_size))
        at = aligned(b * 4 + high * 2 + low, 4 * r1)
        w_hi[at, :] = top
        w_lo[at, :] = rest

    def late(u, _):
        for when, steps in (
            (1, (weigh,)),
            (4, tuple(functools.partial(relay, e) for e in (1, 2, 3))),
            (5, (functools.partial(across, 0),)),
            (7, (functools.partial(across, 1),)),
        ):

            @pl.when(u == when)
            def _():
                with jax.named_scope(f"service_{when}"):
                    for step in steps:
                        step()

        with jax.named_scope("bands_1"):
            c, k = lax.div(u, psi_chunks), lax.rem(u, psi_chunks)
            rows = beta_t[aligned(c, bw), :]
            keep(jnp.dot(rows, psi_v[:, aligned(k, pw)], preferred_element_type=F32), c + 1, k)
        return 0

    lax.fori_loop(0, (beta_chunks - 1) * psi_chunks, late, 0)

    with jax.named_scope("ag_xy"):
        across(2)
        across(3)
    with jax.named_scope("spread_own"):
        for i in range(4):
            spread(band, i // 2, i % 2)
    with jax.named_scope("across"):
        landed(16 * one, recv2c)
        for i in range(4):
            spread(1 - band, i // 2, i % 2)

    def middle3(c):
        near, late = routes[c % 3]
        at = aligned(c, pw)
        landed(near3, recv3.at[c])
        total = fin[pick(near, 0) + (slice(None), at)].reshape(4 * r2, pw)
        for d in peers:
            total += decode(in3[d, :, :, :, at].reshape(4 * r2, pw), in3s[c, d])
        code, scale = encode(total)
        scale3b[c] = scale
        code3b[:, :, :, at] = code.reshape(2, 2, r2, pw)
        mid3[:, :, :, at] = total.reshape(2, 2, r2, pw)
        for d in peers:
            send(
                code3b.at[cell(late, d) + (slice(None), at)], scale3b.at[c],
                end3.at[d, :, at], end3s.at[c, d], recv3b.at[c], device(late, d),
            )

    def product(c):
        at = aligned(c, pw)
        f = jnp.dot(w_hi[...], g_hi[:, at], preferred_element_type=F32)
        f += jnp.dot(w_hi[...], g_lo[:, at], preferred_element_type=F32)
        f += jnp.dot(w_lo[...], g_hi[:, at], preferred_element_type=F32)
        return f + fin[..., at].reshape(2 * cols, pw)

    def share(c, _):
        at = aligned(c, pw)
        with jax.named_scope("share"):
            f = product(c)
            code, scale = encode(f)
            scale3[c] = scale
            code3[..., at] = code.reshape(2, 2, 2, 2, r2, pw)
            fin[..., at] = f.reshape(2, 2, 2, 2, r2, pw)
        for i in range(psi_chunks):
            near = routes[i % 3][0]
            now = pl.ds(i * pw, pw)

            @pl.when(c == i)
            def _():
                for d in peers:
                    send(
                        code3.at[pick(near, d) + (slice(None), now)], scale3.at[i],
                        in3.at[d, :, :, :, now], in3s.at[i, d], recv3.at[i], device(near, d),
                    )

        return 0

    lax.fori_loop(0, psi_chunks, share, 0)
    for c in range(psi_chunks):
        with jax.named_scope(f"mid3_{c}"):
            middle3(c)

    with jax.named_scope("tail"):
        for c in range(psi_chunks):
            at = aligned(c, pw)
            landed(late3, recv3b.at[c])
            total = mid3[cell(routes[c % 3][1], 0) + (slice(None), at)]
            for d in peers:
                total += decode(end3[d, :, at], end3s[c, d])
            out_ref[:, at] = total

    with jax.named_scope("drain"):
        total = beta_chunks * (near1 + late1) + psi_chunks * (near3 + late3) + 31 * one
        counted(total, recv1.at[0]).wait_send()


def fused(n, blk, psi, trial, beta, q_blocks, atom_counts):
    g, cols = trial.shape
    nbands = psi.shape[1]
    p_size = beta.shape[1]
    natom, maxp = q_blocks.shape[:2]
    mp = -(-maxp // 8) * 8
    nd = -(-(2 * maxp - 1) // 8) * 8
    r1, r2 = cols // n, blk // n
    bc, pc = 3, 4
    meter = (2 * (15 * (cols * p_size + blk * nbands) // 16) + 2 * 16 * cols * p_size) // 512 + 1024
    dma = pltpu.SemaphoreType.DMA
    vm = pltpu.VMEM
    out = pl.pallas_call(
        functools.partial(kernel, n, maxp),
        out_shape=jax.ShapeDtypeStruct((r2, nbands), F32),
        in_specs=[pl.BlockSpec(memory_space=pl.ANY)] * 5,
        out_specs=pl.BlockSpec(memory_space=pltpu.VMEM),
        scratch_shapes=[
            vm((g, nbands), BF16),
            vm((g, p_size), BF16),
            vm((g, cols), BF16),
            vm((maxp, maxp, natom), F32),
            vm((1, natom), jnp.int32),
            vm((p_size // bc + blk, g), BF16),
            vm((p_size - p_size // bc, g), BF16),
            vm((cols, g), BF16),
            vm((2, maxp * mp, natom), BF16),
            vm((nd, p_size), F32),
            vm((p_size, nbands), BF16),
            vm((p_size, nbands), BF16),
            vm((blk, p_size), BF16),
            vm((blk, p_size), BF16),
            vm((2, 2, 2, 2, r1, p_size), F32),
            vm((2, 2, 2, 2, r1, p_size), I16),
            vm((bc, 1, p_size // bc), F32),
            vm((4, 2, 2, r1, p_size), I16),
            vm((bc, 4, 1, p_size // bc), F32),
            vm((2, 2, r1, p_size), F32),
            vm((2, 2, r1, p_size), I16),
            vm((bc, 1, p_size // bc), F32),
            vm((4, r1, p_size), I16),
            vm((bc, 4, 1, p_size // bc), F32),
            vm((2, 2, 2, 2, 2, r1, p_size), I16),
            vm((2, 2, 2, 2, 2, 1, 128), F32),
            vm((2, 2, 2, 2, r2, nbands), F32),
            vm((2, 2, 2, 2, r2, nbands), I16),
            vm((pc, 1, nbands // pc), F32),
            vm((4, 2, 2, r2, nbands), I16),
            vm((pc, 4, 1, nbands // pc), F32),
            vm((2, 2, r2, nbands), F32),
            vm((2, 2, r2, nbands), I16),
            vm((pc, 1, nbands // pc), F32),
            vm((4, r2, nbands), I16),
            vm((pc, 4, 1, nbands // pc), F32),
            vm((meter, 1, 128), F32),
            dma((2,)),
            dma,
            dma((bc,)),
            dma((pc,)),
            dma,
            dma,
            dma,
            dma((bc,)),
            dma,
            dma((3,)),
            dma((4,)),
            dma,
            dma((pc,)),
            dma((pc,)),
        ],
        compiler_params=pltpu.CompilerParams(
            collective_id=0, has_side_effects=True, vmem_limit_bytes=62 * 1024 * 1024
        ),
    )(psi, trial, beta, q_blocks.transpose(1, 2, 0), atom_counts.reshape(1, natom))
    return out.T


def q_dense(atom_counts, q_blocks, p_size):
    offsets = jnp.cumsum(atom_counts, dtype=jnp.int32) - atom_counts
    natom, maxp = q_blocks.shape[:2]
    ids = jnp.arange(p_size, dtype=jnp.int32)
    owns = (offsets[None, :] <= ids[:, None]) & (ids[:, None] < (offsets + atom_counts)[None, :])
    pos = jnp.sum(jnp.where(owns, ids[:, None] - offsets[None, :], 0), axis=1)
    atom = jnp.sum(jnp.where(owns, jnp.arange(natom, dtype=jnp.int32)[None, :], 0), axis=1)
    flat = jnp.dot(owns.astype(F32), q_blocks.reshape(natom, maxp * maxp), precision=precise)
    place = pos[:, None] == jnp.arange(maxp, dtype=jnp.int32)[None, :]
    rows = jnp.sum(jnp.where(place[:, :, None], flat.reshape(p_size, maxp, maxp), 0.0), axis=1)
    entries = jnp.dot(rows, place.astype(F32).T, precision=precise)
    return jnp.where(atom[:, None] == atom[None, :], entries, 0.0)


def general(psi, trial, beta, q_blocks, atom_counts):
    own = lax.psum(contract(beta, trial), "ga")
    weighted = jnp.dot(q_dense(atom_counts, q_blocks, beta.shape[1]), own, precision=precise)
    w_hi, w_lo = split2(weighted)
    both = jnp.dot(beta, jnp.concatenate([w_hi, w_lo], axis=1), preferred_element_type=F32)
    cols = trial.shape[1]
    s = both[:, :cols] + both[:, cols:] + trial.astype(F32)
    s_hi, s_lo = split2(lax.all_gather(s, "band", axis=1, tiled=True))
    part = contract(psi, s_hi) + contract(psi, s_lo)
    return lax.psum_scatter(part, "ga", scatter_dimension=1, tiled=True)


def solution(mesh):
    n, bands = mesh.shape["ga"], mesh.shape["band"]

    def shards(psi, trial, beta, q_blocks, atom_counts):
        g, cols = trial.shape
        blk = cols * bands
        fits = (
            bands == 2
            and n == 16
            and cols % 128 == 0
            and cols % (8 * n) == 0
            and blk % (8 * n) == 0
            and g % 4096 == 0
            and beta.shape[1] % 768 == 0
            and psi.shape[1] % 512 == 0
            and q_blocks.shape[0] % 128 == 0
        )
        if fits:
            return fused(n, blk, psi, trial, beta, q_blocks, atom_counts)
        return general(psi, trial, beta, q_blocks, atom_counts)

    in_specs = (P("ga", "band"), P("ga", "band"), P("ga", None), P(), P())
    out_specs = P("band", "ga")
    return jax.shard_map(shards, mesh=mesh, in_specs=in_specs, out_specs=out_specs, check_vma=False)
```
